32 devices in a mesh: dp: 2 (over x), tp: 4 (over z), sp: 4 (over y, core).
Axes of the slice: x: 2, y: 2, z: 4, core: 2. Of those that a mesh axis runs over, the one named last changes fastest.
Arguments:
- x_in: bfloat16 [8192, 4096], P(('dp', 'sp'), 'tp'), parts along dimension 0
- w_qkv: bfloat16 [4096, 12288], P('sp', 'tp')
- w_out: bfloat16 [4096, 4096], P('sp', 'tp')
- seg_ids: int32 [8192], P(('dp', 'sp')), parts along dimension 0
Outputs:
- output: bfloat16 [8192, 4096], P(('dp', 'sp'), 'tp'), parts along dimension 0
There are 2 independent parts. The reference program is written for one: setup_inputs(seed, part) draws one part's arguments, and reference() takes and returns one part's arrays. A program takes and returns all parts, laid end to end along the dimension named above; an argument that names none is the same for every part.
All inputs are finite; a program needn't handle non-finite values.
Results may differ from the reference program's by a relative error of at most 0.00336.
Values are sent between devices in bfloat16 or wider.
A program may use at most 1 GiB of HBM per device.

```python
import jax
import jax.numpy as jnp
from jax import lax

SEQ_LEN = 4096
HIDDEN = 4096
NUM_HEADS = 32
HEAD_DIM = 128
NUM_DOCS = 4
QUERY_BLOCK = 128


def setup_inputs(seed: int = 0, part: int = 0) -> dict:
    key_qkv, key_out = jax.random.split(jax.random.key(seed))
    part_key = jax.random.fold_in(jax.random.key(seed + 1), part)
    key_x, key_seg = jax.random.split(part_key)
    x_in = jax.random.normal(key_x, (SEQ_LEN, HIDDEN), jnp.float32)
    w_qkv = jax.random.normal(key_qkv, (HIDDEN, 3 * HIDDEN), jnp.float32) * (1.5 / HIDDEN ** 0.5)
    w_out = jax.random.normal(key_out, (HIDDEN, HIDDEN), jnp.float32) * (2.0 / HIDDEN ** 0.5)
    doc_starts = jax.random.permutation(key_seg, SEQ_LEN - 1)[: NUM_DOCS - 1] + 1
    positions = jnp.arange(SEQ_LEN, dtype=jnp.int32)
    seg_ids = jnp.sum((positions[:, None] >= doc_starts[None, :]).astype(jnp.int32), axis=1)
    return {"x_in": x_in.astype(jnp.bfloat16), "w_qkv": w_qkv.astype(jnp.bfloat16), "w_out": w_out.astype(jnp.bfloat16), "seg_ids": seg_ids.astype(jnp.int32)}


def reference(x_in, w_qkv, w_out, seg_ids):
    qkv_proj = jnp.dot(x_in, w_qkv, preferred_element_type=jnp.float32).astype(jnp.bfloat16)
    qkv_proj = qkv_proj.reshape(SEQ_LEN, NUM_HEADS, 3, HEAD_DIM).transpose(1, 2, 0, 3)
    n_blocks = SEQ_LEN // QUERY_BLOCK
    positions = jnp.arange(SEQ_LEN, dtype=jnp.int32)
    pos_query = positions.reshape(n_blocks, QUERY_BLOCK)
    seg_query = seg_ids.reshape(n_blocks, QUERY_BLOCK)
    score_scale = 1.0 / HEAD_DIM ** 0.5

    def one_head(head_qkv):
        key_head = head_qkv[1]
        value_head = head_qkv[2]
        query_blocks = head_qkv[0].reshape(n_blocks, QUERY_BLOCK, HEAD_DIM)

        def one_block(block_args):
            query_blk, pos_blk, seg_blk = block_args
            scores = jnp.dot(query_blk, key_head.T, preferred_element_type=jnp.float32) * score_scale
            allowed = (positions[None, :] <= pos_blk[:, None]) & (seg_ids[None, :] == seg_blk[:, None])
            scores = jnp.where(allowed, scores, -jnp.inf)
            prob_blk = jax.nn.softmax(scores, axis=-1).astype(jnp.bfloat16)
            return jnp.dot(prob_blk, value_head, preferred_element_type=jnp.float32).astype(jnp.bfloat16)

        return lax.map(one_block, (query_blocks, pos_query, seg_query)).reshape(SEQ_LEN, HEAD_DIM)

    context = lax.map(one_head, qkv_proj)
    context = context.transpose(1, 0, 2).reshape(SEQ_LEN, HIDDEN)
    return jnp.dot(context, w_out, preferred_element_type=jnp.float32).astype(jnp.bfloat16)
```

```python
import functools

import jax
import jax.numpy as jnp
from jax import lax
from jax.experimental import pallas as pl
from jax.experimental.pallas import tpu as pltpu
from jax.sharding import PartitionSpec as P

HEAD_DIM = 128
NT = 4
NR = 8
NP = 4
LOG2E = 1.4426950408889634
MIB = 1024 * 1024


def _mo(i, n):
    return pl.multiple_of(i * n, n)


def _gather_dot(qkv, x_hbm, w_hbm, seg_hbm, *refs):
    if qkv:
        q_ref, kv_all, seg_all = refs[:3]
        refs = refs[3:]
    else:
        (y_ref,) = refs[:1]
        refs = refs[1:]
    xg, wg = refs[:2]
    refs = refs[2:]
    if qkv:
        kv = refs[0]
        refs = refs[1:]
    loc, xs, xl, xr, ws_own, ws_y, ws_x, ws_f, wr_own, wr_y, wr_x, wr_f = refs[:12]
    if qkv:
        kv_send, kv_yr, kv_cr, kv_fs, kv_fr, seg_s, seg_r = refs[12:]

    R, C = x_hbm.shape
    N = w_hbm.shape[1]
    RC, NG, NH = R // NR, N // NP, N // (2 * NP)
    d, t, s = lax.axis_index("dp"), lax.axis_index("tp"), lax.axis_index("sp")
    yc, c = s // 2, s % 2
    sib, ynb, diag = s + 1 - 2 * c, s + 2 - 4 * yc, (2 - 2 * yc) + (1 - c)
    mesh_id = pl.DeviceIdType.MESH
    to_sib, to_y, to_diag = (d, t, sib), (d, t, ynb), (d, t, diag)
    to_x = (1 - d, t, s)
    to_right, to_left = (d, t + 1, s), (d, t - 1, s)
    has_right, has_left = t < NT - 1, t > 0

    bar = pltpu.get_barrier_semaphore()

    def greet(who):
        pl.semaphore_signal(bar, inc=1, device_id=who, device_id_type=mesh_id)

    greet(to_sib)
    greet(to_y)
    greet(to_x)
    if qkv:
        greet(to_diag)

    @pl.when(has_right)
    def _():
        greet(to_right)

    @pl.when(has_left)
    def _():
        greet(to_left)

    base = 4 if qkv else 3

    @pl.when(has_right & has_left)
    def _():
        pl.semaphore_wait(bar, base + 2)

    @pl.when(jnp.logical_not(has_right & has_left))
    def _():
        pl.semaphore_wait(bar, base + 1)

    def remote(src, dst, send, recv, who):
        return pltpu.make_async_remote_copy(src, dst, send, recv, device_id=who, device_id_type=mesh_id)

    def w_own(p):
        cols = pl.ds(p * NG, NG)
        return remote(w_hbm.at[:, cols], wg.at[s, :, cols], ws_own.at[p], wr_own.at[p], to_sib)

    def w_own_in(p):
        cols = pl.ds(p * NG, NG)
        return remote(w_hbm.at[:, cols], wg.at[sib, :, cols], ws_own.at[p], wr_own.at[p], to_sib)

    def mine(p):
        return pl.ds(_mo(2 * p + d, NH), NH)

    def other(p):
        return pl.ds(_mo(2 * p + 1 - d, NH), NH)

    def w_y(p):
        return remote(w_hbm.at[:, mine(p)], wg.at[s, :, mine(p)], ws_y.at[p], wr_y.at[p], to_y)

    def w_y_in(p):
        return remote(w_hbm.at[:, mine(p)], wg.at[ynb, :, mine(p)], ws_y.at[p], wr_y.at[p], to_y)

    def w_x(p):
        return remote(wg.at[ynb, :, mine(p)], wg.at[ynb, :, mine(p)], ws_x.at[p], wr_x.at[p], to_x)

    def w_x_in(p):
        return remote(wg.at[ynb, :, other(p)], wg.at[ynb, :, other(p)], ws_x.at[p], wr_x.at[p], to_x)

    def w_f(p, which):
        cols = mine(p) if which == 0 else other(p)
        return remote(wg.at[ynb, :, cols], wg.at[ynb, :, cols], ws_f.at[which, p], wr_f.at[which, p], to_sib)

    def w_f_in(p, which):
        cols = mine(p) if which == 0 else other(p)
        return remote(wg.at[diag, :, cols], wg.at[diag, :, cols], ws_f.at[which, p], wr_f.at[which, p], to_sib)

    def rows(r):
        return pl.ds(_mo(r, RC), RC)

    def x_own(r, way):
        recv = xl if way == 0 else xr
        return remote(x_hbm.at[rows(r)], xg.at[t, rows(r)], xs.at[way, 0, r], recv.at[0, r], to_right if way == 0 else to_left)

    def x_arrive(r, way, dist):
        k = t - dist if way == 0 else t + dist
        recv = xl if way == 0 else xr
        return remote(xg.at[k, rows(r)], xg.at[k, rows(r)], xs.at[way, 0, r], recv.at[dist - 1, r], to_right if way == 0 else to_left)

    def x_forward(r, way, dist):
        k = t - dist if way == 0 else t + dist
        recv = xl if way == 0 else xr
        return remote(xg.at[k, rows(r)], xg.at[k, rows(r)], xs.at[way, dist, r], recv.at[dist, r], to_right if way == 0 else to_left)

    def send_own_x(r):
        @pl.when(has_right)
        def _():
            x_own(r, 0).start()

        @pl.when(has_left)
        def _():
            x_own(r, 1).start()

    def relay_x(r):
        for dist in range(1, NT):
            for way in range(2):
                here = (t >= dist) if way == 0 else (t <= NT - 1 - dist)

                @pl.when(here)
                def _():
                    x_arrive(r, way, dist).wait_recv()
                    if dist < NT - 1:
                        @pl.when(has_right if way == 0 else has_left)
                        def _():
                            x_forward(r, way, dist).start()

    own_x = pltpu.make_async_copy(x_hbm, xg.at[t], loc.at[0])
    own_w = pltpu.make_async_copy(w_hbm, wg.at[s], loc.at[1])
    for r in range(2):
        send_own_x(r)
    for p in range(NP):
        w_y(p).start()
    for p in range(NP):
        w_own(p).start()
    own_x.start()
    own_w.start()
    if qkv:
        own_seg = pltpu.make_async_copy(seg_hbm, seg_all.at[s], loc.at[3])
        own_seg.start()
        peers = ((to_sib, sib), (to_y, ynb), (to_diag, diag))

        def seg_out(i):
            return remote(seg_hbm, seg_all.at[s], seg_s.at[i], seg_r.at[i], peers[i][0])

        def seg_in(i):
            return remote(seg_hbm, seg_all.at[peers[i][1]], seg_s.at[i], seg_r.at[i], peers[i][0])

        for i in range(3):
            seg_out(i).start()

    def unit(r, p):
        cols = pl.ds(_mo(p, NG), NG)
        acc = jnp.dot(xg[0, rows(r), :], wg[0, :, cols], preferred_element_type=jnp.float32)
        for k in range(1, NT):
            acc += jnp.dot(xg[k, rows(r), :], wg[k, :, cols], preferred_element_type=jnp.float32)
        out = acc.astype(jnp.bfloat16)
        if qkv:
            for h in range(2):
                at = 3 * HEAD_DIM * h
                q_ref[rows(r), pl.ds(pl.multiple_of(p * (2 * HEAD_DIM) + h * HEAD_DIM, HEAD_DIM), HEAD_DIM)] = out[:, at : at + HEAD_DIM]
                kv[rows(r), pl.ds(_mo(2 * p + h, 2 * HEAD_DIM), 2 * HEAD_DIM)] = out[:, at + HEAD_DIM : at + 3 * HEAD_DIM]
        else:
            y_ref[rows(r), cols] = out

    def kv_cols(p):
        return pl.ds(_mo(p, 4 * HEAD_DIM), 4 * HEAD_DIM)

    def kv_unit(r, p, who, send, recv):
        return remote(kv.at[rows(r), kv_cols(p)], kv_all.at[s, rows(r), kv_cols(p)], send, recv, who)

    def send_unit(r, p):
        pltpu.make_async_copy(kv.at[rows(r), kv_cols(p)], kv_all.at[s, rows(r), kv_cols(p)], loc.at[2]).start()

        @pl.when(yc == 0)
        def _():
            kv_unit(r, p, to_y, kv_send.at[0], kv_yr.at[r]).start()

        @pl.when(c == 0)
        def _():
            kv_unit(r, p, to_sib, kv_send.at[1], kv_cr.at[r]).start()

    def do_units(work):
        for n, f in work:
            def body(u, z, f=f):
                unit(*f(u))
                return z
            lax.fori_loop(0, n, body, 0)
        if qkv:
            for n, f in work:
                def body(u, z, f=f):
                    send_unit(*f(u))
                    return z
                lax.fori_loop(0, n, body, 0)

    def kv_row(r, owner, who, send, recv):
        return remote(kv_all.at[owner, rows(r)], kv_all.at[owner, rows(r)], send, recv, who)

    def pass_kv(r):
        if qkv:
            @pl.when(yc == 1)
            def _():
                kv_row(r, ynb, to_y, kv_fs.at[r], kv_yr.at[r]).wait_recv()
                kv_row(r, ynb, to_sib, kv_fs.at[r], kv_fr.at[r]).start()

    def relay_w(i):
        if i < NP:
            w_y_in(i).wait_recv()
            w_x(i).start()
            w_f(i, 0).start()
        if 1 <= i <= NP:
            w_x_in(i - 1).wait_recv()
            w_f(i - 1, 1).start()
            p = i - 1
            if p == 0:
                own_x.wait()
                own_w.wait()
            w_own_in(p).wait_recv()
            w_f_in(p, 0).wait_recv()
            w_f_in(p, 1).wait_recv()

    for i in range(NP + 1):
        relay_x(i)
        send_own_x(i + 2)
        relay_w(i)
        if i == 2:
            do_units([(6, lambda u: (u // 2, u % 2))])
        if i == 3:
            do_units([(2, lambda u: (3, u)), (4, lambda u: (u, 2))])
        if i == 4:
            do_units([(3, lambda u: (4, u)), (5, lambda u: (u, 3))])

    def late(i, z):
        relay_x(i)

        @pl.when(i + 2 < NR)
        def _():
            send_own_x(i + 2)

        pass_kv(2 * (i - NP - 1))
        pass_kv(2 * (i - NP - 1) + 1)
        do_units([(NP, lambda u: (i, u))])
        return z

    lax.fori_loop(NP + 1, NR, late, 0)

    for p in range(NP):
        w_own(p).wait_send()
        w_y(p).wait_send()
        w_x(p).wait_send()
        w_f(p, 0).wait_send()
        w_f(p, 1).wait_send()

    def drain_x(r, z):
        @pl.when(has_right)
        def _():
            x_own(r, 0).wait_send()
            for dist in range(1, NT - 1):
                @pl.when(t >= dist)
                def _():
                    x_forward(r, 0, dist).wait_send()

        @pl.when(has_left)
        def _():
            x_own(r, 1).wait_send()
            for dist in range(1, NT - 1):
                @pl.when(t <= NT - 1 - dist)
                def _():
                    x_forward(r, 1, dist).wait_send()

        return z

    lax.fori_loop(0, NR, drain_x, 0)
    if qkv:
        pass_kv(6)
        pass_kv(7)
        own_seg.wait()
        for i in range(3):
            seg_out(i).wait_send()
            seg_in(i).wait_recv()
        pltpu.make_async_copy(kv, kv_all.at[s], loc.at[2]).wait()

        @pl.when(yc == 0)
        def _():
            remote(kv, kv_all.at[s], kv_send.at[0], kv_yr.at[0], to_y).wait_send()

        @pl.when(c == 0)
        def _():
            remote(kv, kv_all.at[s], kv_send.at[1], kv_cr.at[0], to_sib).wait_send()

        def drain_kv(r, z):
            @pl.when(c == 1)
            def _():
                kv_row(r, sib, to_sib, kv_fs.at[r], kv_cr.at[r]).wait_recv()

            @pl.when(yc == 1)
            def _():
                kv_row(r, ynb, to_sib, kv_fs.at[r], kv_fr.at[r]).wait_send()
                kv_row(r, diag, to_sib, kv_fs.at[r], kv_fr.at[r]).wait_recv()

            return z

        lax.fori_loop(0, NR, drain_kv, 0)


def _gather_call(qkv, x, w, seg):
    R, C = x.shape
    N = w.shape[1]
    dma = pltpu.SemaphoreType.DMA
    hbm = pl.BlockSpec(memory_space=pltpu.HBM)
    vmem = pl.BlockSpec(memory_space=pltpu.VMEM)
    bf16 = jnp.bfloat16
    scratch = [pltpu.VMEM((NT, R, C), bf16), pltpu.VMEM((NT, C, N), bf16)]
    if qkv:
        heads = N // (3 * HEAD_DIM)
        out_shape = (
            jax.ShapeDtypeStruct((R, heads * HEAD_DIM), bf16),
            jax.ShapeDtypeStruct((NT, R, 2 * heads * HEAD_DIM), bf16),
            jax.ShapeDtypeStruct((NT,) + seg.shape, jnp.int32),
        )
        out_specs = (vmem, hbm, hbm)
        scratch.append(pltpu.VMEM((R, 2 * heads * HEAD_DIM), bf16))
    else:
        out_shape = jax.ShapeDtypeStruct((R, N), bf16)
        out_specs = vmem
    scratch += [dma((4,)), dma((2, 3, NR)), dma((3, NR)), dma((3, NR)), dma((NP,)), dma((NP,)), dma((NP,)), dma((2, NP)),
                dma((NP,)), dma((NP,)), dma((NP,)), dma((2, NP))]
    if qkv:
        scratch += [dma((2,)), dma((NR,)), dma((NR,)), dma((NR,)), dma((NR,)), dma((3,)), dma((3,))]
    return pl.pallas_call(
        functools.partial(_gather_dot, qkv),
        out_shape=out_shape,
        in_specs=[hbm, hbm, hbm],
        out_specs=out_specs,
        scratch_shapes=scratch,
        compiler_params=pltpu.CompilerParams(collective_id=0 if qkv else 1, has_side_effects=True, vmem_limit_bytes=60 * MIB),
        cost_estimate=pl.CostEstimate(flops=2 * R * NT * C * N, bytes_accessed=2 * NT * (R * C + C * N), transcendentals=0),
        name="qkv_dot" if qkv else "out_dot",
    )(x, w, seg)


def _attention(BQ, BK, s_ref, seg_ref, q_ref, kv_ref, o_ref, st_ref, sc_ref, m_ref, l_ref, acc_ref):
    R = q_ref.shape[0]
    s = s_ref[0]
    seg = seg_ref[...]
    scale = LOG2E / HEAD_DIM ** 0.5
    for doc in range(1, 4):
        st_ref[doc] = jnp.sum((seg < doc).astype(jnp.int32))

    def doc_start(row):
        out = jnp.zeros_like(row)
        for doc in range(1, 4):
            start = st_ref[doc]
            out = jnp.where(start <= row, jnp.maximum(out, start), out)
        return out

    def lane_groups(a, op):
        out = a[:, :HEAD_DIM]
        for g in range(1, a.shape[1] // HEAD_DIM):
            out = op(out, a[:, HEAD_DIM * g : HEAD_DIM * (g + 1)])
        return out

    def q_block(b, z):
        row0 = s * R + b * BQ
        q_at = pl.ds(_mo(b, BQ), BQ)
        lo = doc_start(row0) // BK
        hi = (row0 + BQ - 1) // BK + 1
        full_lo = jnp.clip((doc_start(row0 + BQ - 1) + BK - 1) // BK, lo, hi)
        full_hi = jnp.clip((row0 + 1) // BK, full_lo, hi)
        m_ref[...] = jnp.full(m_ref.shape, -3e38, jnp.float32)
        l_ref[...] = jnp.zeros(l_ref.shape, jnp.float32)
        acc_ref[...] = jnp.zeros(acc_ref.shape, jnp.float32)

        def scores(j, z, masked):
            k_at = pl.ds(_mo(j, BK), BK)
            if masked:
                row_id = row0 + lax.broadcasted_iota(jnp.int32, (BQ, 1), 0)
                key_id = j * BK + lax.broadcasted_iota(jnp.int32, (BQ, BK), 1)
                seen = (key_id <= row_id) & (key_id >= doc_start(row_id))
            for h in range(2):
                q = q_ref[q_at, HEAD_DIM * h : HEAD_DIM * (h + 1)]
                k = kv_ref[k_at, 2 * HEAD_DIM * h : 2 * HEAD_DIM * h + HEAD_DIM]
                sc = lax.dot_general(q, k, (((1,), (1,)), ((), ())), preferred_element_type=jnp.float32)
                if masked:
                    sc = jnp.where(seen, sc, -jnp.inf)
                sc_ref[h, j] = sc
                m_ref[h] = jnp.maximum(m_ref[h], lane_groups(sc, jnp.maximum))
            return z

        def weights(j, z):
            for h in range(2):
                m = m_ref[h]
                e = jnp.exp2((sc_ref[h, j] - jnp.concatenate([m] * (BK // HEAD_DIM), axis=1)) * scale)
                sc_ref[h, j] = e
                l_ref[h] = l_ref[h] + lane_groups(e, jnp.add)
            return z

        def values(j, z):
            k_at = pl.ds(_mo(j, BK), BK)
            for h in range(2):
                v = kv_ref[k_at, 2 * HEAD_DIM * h + HEAD_DIM : 2 * HEAD_DIM * (h + 1)]
                p = (sc_ref[h, j] * jnp.concatenate([l_ref[h]] * (BK // HEAD_DIM), axis=1)).astype(jnp.bfloat16)
                acc_ref[h] = acc_ref[h] + jnp.dot(p, v, preferred_element_type=jnp.float32)
            return z

        lax.fori_loop(lo, full_lo, functools.partial(scores, masked=True), 0)
        lax.fori_loop(full_lo, full_hi, functools.partial(scores, masked=False), 0)
        lax.fori_loop(full_hi, hi, functools.partial(scores, masked=True), 0)
        for h in range(2):
            m_ref[h] = jnp.broadcast_to(jnp.max(m_ref[h], axis=1, keepdims=True), (BQ, HEAD_DIM))
        lax.fori_loop(lo, hi, weights, 0)
        for h in range(2):
            l_ref[h] = jnp.broadcast_to(1.0 / jnp.sum(l_ref[h], axis=1, keepdims=True), (BQ, HEAD_DIM))
        lax.fori_loop(lo, hi, values, 0)
        for h in range(2):
            o_ref[q_at, HEAD_DIM * h : HEAD_DIM * (h + 1)] = acc_ref[h].astype(jnp.bfloat16)
        return z

    lax.fori_loop(0, R // BQ, q_block, 0)


def _attention_call(q, kv_all, seg_all):
    R, cols = q.shape
    rows = NT * R
    BQ, BK = min(512, R), min(512, R)
    s = lax.axis_index("sp").astype(jnp.int32).reshape(1)
    return pl.pallas_call(
        functools.partial(_attention, BQ, BK),
        out_shape=jax.ShapeDtypeStruct((R, cols), jnp.bfloat16),
        grid_spec=pltpu.PrefetchScalarGridSpec(
            num_scalar_prefetch=1,
            grid=(cols // (2 * HEAD_DIM),),
            in_specs=[
                pl.BlockSpec(seg_all.shape, lambda p, s: (0, 0)),
                pl.BlockSpec((R, 2 * HEAD_DIM), lambda p, s: (0, p)),
                pl.BlockSpec((rows, 4 * HEAD_DIM), lambda p, s: (0, p)),
            ],
            out_specs=pl.BlockSpec((R, 2 * HEAD_DIM), lambda p, s: (0, p)),
            scratch_shapes=[
                pltpu.SMEM((4,), jnp.int32),
                pltpu.VMEM((2, rows // BK, BQ, BK), jnp.float32),
                pltpu.VMEM((2, BQ, HEAD_DIM), jnp.float32),
                pltpu.VMEM((2, BQ, HEAD_DIM), jnp.float32),
                pltpu.VMEM((2, BQ, HEAD_DIM), jnp.float32),
            ],
        ),
        compiler_params=pltpu.CompilerParams(vmem_limit_bytes=48 * MIB),
        cost_estimate=pl.CostEstimate(flops=2 * R * rows * cols, bytes_accessed=4 * rows * cols, transcendentals=R * rows * cols // 256),
        name="attention",
    )(s, seg_all, q, kv_all)


def solution(mesh):
    def local_block(x_blk, wqkv_blk, wout_blk, seg_blk):
        R = x_blk.shape[0]
        seg = seg_blk.reshape(-1, 128)
        q, kv_all, seg_all = _gather_call(True, x_blk, wqkv_blk, seg)
        context = _attention_call(q, kv_all.reshape(NT * R, -1), seg_all.reshape(-1, 128))
        return _gather_call(False, context, wout_blk, seg)

    row_spec = P(("dp", "sp"), "tp")
    return jax.shard_map(local_block, mesh=mesh, in_specs=(row_spec, P("sp", "tp"), P("sp", "tp"), P(("dp", "sp"))), out_specs=row_spec, check_vma=False)
```

```python
import functools

import jax
import jax.numpy as jnp
from jax import lax
from jax.experimental import pallas as pl
from jax.experimental.pallas import tpu as pltpu
from jax.sharding import PartitionSpec as P

HEAD_DIM = 128
NT = 4
NR = 8
NP = 4
LOG2E = 1.4426950408889634
MIB = 1024 * 1024


def _mo(i, n):
    return pl.multiple_of(i * n, n)


def _gather_dot(qkv, x_hbm, w_hbm, seg_hbm, *refs):
    if qkv:
        q_ref, kv_all, seg_all = refs[:3]
        refs = refs[3:]
    else:
        (y_ref,) = refs[:1]
        refs = refs[1:]
    xg, wg = refs[:2]
    refs = refs[2:]
    if qkv:
        kv = refs[0]
        refs = refs[1:]
    loc, xs, xl, xr, ws_own, ws_y, ws_x, ws_f, wr_own, wr_y, wr_x, wr_f = refs[:12]
    if qkv:
        kv_send, kv_yr, kv_cr, kv_fs, kv_fr, seg_s, seg_r = refs[12:]

    R, C = x_hbm.shape
    N = w_hbm.shape[1]
    RC, NG, NH = R // NR, N // NP, N // (2 * NP)
    d, t, s = lax.axis_index("dp"), lax.axis_index("tp"), lax.axis_index("sp")
    yc, c = s // 2, s % 2
    sib, ynb, diag = s + 1 - 2 * c, s + 2 - 4 * yc, (2 - 2 * yc) + (1 - c)
    mesh_id = pl.DeviceIdType.MESH
    to_sib, to_y, to_diag = (d, t, sib), (d, t, ynb), (d, t, diag)
    to_x = (1 - d, t, s)
    to_right, to_left = (d, t + 1, s), (d, t - 1, s)
    has_right, has_left = t < NT - 1, t > 0

    bar = pltpu.get_barrier_semaphore()

    def greet(who):
        pl.semaphore_signal(bar, inc=1, device_id=who, device_id_type=mesh_id)

    greet(to_sib)
    greet(to_y)
    greet(to_x)
    if qkv:
        greet(to_diag)

    @pl.when(has_right)
    def _():
        greet(to_right)

    @pl.when(has_left)
    def _():
        greet(to_left)

    base = 4 if qkv else 3

    @pl.when(has_right & has_left)
    def _():
        pl.semaphore_wait(bar, base + 2)

    @pl.when(jnp.logical_not(has_right & has_left))
    def _():
        pl.semaphore_wait(bar, base + 1)

    def remote(src, dst, send, recv, who):
        return pltpu.make_async_remote_copy(src, dst, send, recv, device_id=who, device_id_type=mesh_id)

    def w_own(p):
        cols = pl.ds(p * NG, NG)
        return remote(w_hbm.at[:, cols], wg.at[s, :, cols], ws_own.at[p], wr_own.at[p], to_sib)

    def w_own_in(p):
        cols = pl.ds(p * NG, NG)
        return remote(w_hbm.at[:, cols], wg.at[sib, :, cols], ws_own.at[p], wr_own.at[p], to_sib)

    def mine(p):
        return pl.ds(_mo(2 * p + d, NH), NH)

    def other(p):
        return pl.ds(_mo(2 * p + 1 - d, NH), NH)

    def w_y(p):
        return remote(w_hbm.at[:, mine(p)], wg.at[s, :, mine(p)], ws_y.at[p], wr_y.at[p], to_y)

    def w_y_in(p):
        return remote(w_hbm.at[:, mine(p)], wg.at[ynb, :, mine(p)], ws_y.at[p], wr_y.at[p], to_y)

    def w_x(p):
        return remote(wg.at[ynb, :, mine(p)], wg.at[ynb, :, mine(p)], ws_x.at[p], wr_x.at[p], to_x)

    def w_x_in(p):
        return remote(wg.at[ynb, :, other(p)], wg.at[ynb, :, other(p)], ws_x.at[p], wr_x.at[p], to_x)

    def w_f(p, which):
        cols = mine(p) if which == 0 else other(p)
        return remote(wg.at[ynb, :, cols], wg.at[ynb, :, cols], ws_f.at[which, p], wr_f.at[which, p], to_sib)

    def w_f_in(p, which):
        cols = mine(p) if which == 0 else other(p)
        return remote(wg.at[diag, :, cols], wg.at[diag, :, cols], ws_f.at[which, p], wr_f.at[which, p], to_sib)

    def rows(r):
        return pl.ds(_mo(r, RC), RC)

    def x_own(r, way):
        recv = xl if way == 0 else xr
        return remote(x_hbm.at[rows(r)], xg.at[t, rows(r)], xs.at[way, 0, r], recv.at[0, r], to_right if way == 0 else to_left)

    def x_arrive(r, way, dist):
        k = t - dist if way == 0 else t + dist
        recv = xl if way == 0 else xr
        return remote(xg.at[k, rows(r)], xg.at[k, rows(r)], xs.at[way, 0, r], recv.at[dist - 1, r], to_right if way == 0 else to_left)

    def x_forward(r, way, dist):
        k = t - dist if way == 0 else t + dist
        recv = xl if way == 0 else xr
        return remote(xg.at[k, rows(r)], xg.at[k, rows(r)], xs.at[way, dist, r], recv.at[dist, r], to_right if way == 0 else to_left)

    def send_own_x(r):
        @pl.when(has_right)
        def _():
            x_own(r, 0).start()

        @pl.when(has_left)
        def _():
            x_own(r, 1).start()

    def relay_x(r):
        for dist in range(1, NT):
            for way in range(2):
                here = (t >= dist) if way == 0 else (t <= NT - 1 - dist)

                @pl.when(here)
                def _():
                    x_arrive(r, way, dist).wait_recv()
                    if dist < NT - 1:
                        @pl.when(has_right if way == 0 else has_left)
                        def _():
                            x_forward(r, way, dist).start()

    own_x = pltpu.make_async_copy(x_hbm, xg.at[t], loc.at[0])
    own_w = pltpu.make_async_copy(w_hbm, wg.at[s], loc.at[1])
    for r in range(2):
        send_own_x(r)
    for p in range(NP):
        w_y(p).start()
    for p in range(NP):
        w_own(p).start()
    own_x.start()
    own_w.start()
    if qkv:
        own_seg = pltpu.make_async_copy(seg_hbm, seg_all.at[s], loc.at[3])
        own_seg.start()
        peers = ((to_sib, sib), (to_y, ynb), (to_diag, diag))

        def seg_out(i):
            return remote(seg_hbm, seg_all.at[s], seg_s.at[i], seg_r.at[i], peers[i][0])

        def seg_in(i):
            return remote(seg_hbm, seg_all.at[peers[i][1]], seg_s.at[i], seg_r.at[i], peers[i][0])

        for i in range(3):
            seg_out(i).start()

    def unit(r, p):
        cols = pl.ds(_mo(p, NG), NG)
        acc = jnp.dot(xg[0, rows(r), :], wg[0, :, cols], preferred_element_type=jnp.float32)
        for k in range(1, NT):
            acc += jnp.dot(xg[k, rows(r), :], wg[k, :, cols], preferred_element_type=jnp.float32)
        out = acc.astype(jnp.bfloat16)
        if qkv:
            for h in range(2):
                at = 3 * HEAD_DIM * h
                q_ref[rows(r), pl.ds(pl.multiple_of(p * (2 * HEAD_DIM) + h * HEAD_DIM, HEAD_DIM), HEAD_DIM)] = out[:, at : at + HEAD_DIM]
                kv[rows(r), pl.ds(_mo(2 * p + h, 2 * HEAD_DIM), 2 * HEAD_DIM)] = out[:, at + HEAD_DIM : at + 3 * HEAD_DIM]
        else:
            y_ref[rows(r), cols] = out

    def kv_cols(p):
        return pl.ds(_mo(p, 4 * HEAD_DIM), 4 * HEAD_DIM)

    def kv_unit(r, p, who, send, recv):
        return remote(kv.at[rows(r), kv_cols(p)], kv_all.at[s, rows(r), kv_cols(p)], send, recv, who)

    def send_unit(r, p):
        pltpu.make_async_copy(kv.at[rows(r), kv_cols(p)], kv_all.at[s, rows(r), kv_cols(p)], loc.at[2]).start()

        @pl.when(yc == 0)
        def _():
            kv_unit(r, p, to_y, kv_send.at[0], kv_yr.at[r]).start()

        @pl.when(c == 0)
        def _():
            kv_unit(r, p, to_sib, kv_send.at[1], kv_cr.at[r]).start()

    def do_units(work):
        for n, f in work:
            def body(u, z, f=f):
                unit(*f(u))
                return z
            lax.fori_loop(0, n, body, 0)
        if qkv:
            for n, f in work:
                def body(u, z, f=f):
                    send_unit(*f(u))
                    return z
                lax.fori_loop(0, n, body, 0)

    def kv_row(r, owner, who, send, recv):
        return remote(kv_all.at[owner, rows(r)], kv_all.at[owner, rows(r)], send, recv, who)

    def pass_kv(r):
        if qkv:
            @pl.when(yc == 1)
            def _():
                kv_row(r, ynb, to_y, kv_fs.at[r], kv_yr.at[r]).wait_recv()
                kv_row(r, ynb, to_sib, kv_fs.at[r], kv_fr.at[r]).start()

    def relay_w(i):
        if i < NP:
            w_y_in(i).wait_recv()
            w_x(i).start()
            w_f(i, 0).start()
        if 1 <= i <= NP:
            w_x_in(i - 1).wait_recv()
            w_f(i - 1, 1).start()
            p = i - 1
            if p == 0:
                own_x.wait()
                own_w.wait()
            w_own_in(p).wait_recv()
            w_f_in(p, 0).wait_recv()
            w_f_in(p, 1).wait_recv()

    for i in range(NP + 1):
        relay_x(i)
        send_own_x(i + 2)
        relay_w(i)
        if i == 2:
            do_units([(6, lambda u: (u // 2, u % 2))])
        if i == 3:
            do_units([(2, lambda u: (3, u)), (4, lambda u: (u, 2))])
        if i == 4:
            do_units([(3, lambda u: (4, u)), (5, lambda u: (u, 3))])

    def late(i, z):
        relay_x(i)

        @pl.when(i + 2 < NR)
        def _():
            send_own_x(i + 2)

        pass_kv(2 * (i - NP - 1))
        pass_kv(2 * (i - NP - 1) + 1)
        do_units([(NP, lambda u: (i, u))])
        return z

    lax.fori_loop(NP + 1, NR, late, 0)

    for p in range(NP):
        w_own(p).wait_send()
        w_y(p).wait_send()
        w_x(p).wait_send()
        w_f(p, 0).wait_send()
        w_f(p, 1).wait_send()

    def drain_x(r, z):
        @pl.when(has_right)
        def _():
            x_own(r, 0).wait_send()
            for dist in range(1, NT - 1):
                @pl.when(t >= dist)
                def _():
                    x_forward(r, 0, dist).wait_send()

        @pl.when(has_left)
        def _():
            x_own(r, 1).wait_send()
            for dist in range(1, NT - 1):
                @pl.when(t <= NT - 1 - dist)
                def _():
                    x_forward(r, 1, dist).wait_send()

        return z

    lax.fori_loop(0, NR, drain_x, 0)
    if qkv:
        pass_kv(6)
        pass_kv(7)
        own_seg.wait()
        for i in range(3):
            seg_out(i).wait_send()
            seg_in(i).wait_recv()
        pltpu.make_async_copy(kv, kv_all.at[s], loc.at[2]).wait()

        @pl.when(yc == 0)
        def _():
            remote(kv, kv_all.at[s], kv_send.at[0], kv_yr.at[0], to_y).wait_send()

        @pl.when(c == 0)
        def _():
            remote(kv, kv_all.at[s], kv_send.at[1], kv_cr.at[0], to_sib).wait_send()

        def drain_kv(r, z):
            @pl.when(c == 1)
            def _():
                kv_row(r, sib, to_sib, kv_fs.at[r], kv_cr.at[r]).wait_recv()

            @pl.when(yc == 1)
            def _():
                kv_row(r, ynb, to_sib, kv_fs.at[r], kv_fr.at[r]).wait_send()
                kv_row(r, diag, to_sib, kv_fs.at[r], kv_fr.at[r]).wait_recv()

            return z

        lax.fori_loop(0, NR, drain_kv, 0)


def _gather_call(qkv, x, w, seg):
    R, C = x.shape
    N = w.shape[1]
    dma = pltpu.SemaphoreType.DMA
    hbm = pl.BlockSpec(memory_space=pltpu.HBM)
    vmem = pl.BlockSpec(memory_space=pltpu.VMEM)
    bf16 = jnp.bfloat16
    scratch = [pltpu.VMEM((NT, R, C), bf16), pltpu.VMEM((NT, C, N), bf16)]
    if qkv:
        heads = N // (3 * HEAD_DIM)
        out_shape = (
            jax.ShapeDtypeStruct((R, heads * HEAD_DIM), bf16),
            jax.ShapeDtypeStruct((NT, R, 2 * heads * HEAD_DIM), bf16),
            jax.ShapeDtypeStruct((NT,) + seg.shape, jnp.int32),
        )
        out_specs = (vmem, hbm, hbm)
        scratch.append(pltpu.VMEM((R, 2 * heads * HEAD_DIM), bf16))
    else:
        out_shape = jax.ShapeDtypeStruct((R, N), bf16)
        out_specs = vmem
    scratch += [dma((4,)), dma((2, 3, NR)), dma((3, NR)), dma((3, NR)), dma((NP,)), dma((NP,)), dma((NP,)), dma((2, NP)),
                dma((NP,)), dma((NP,)), dma((NP,)), dma((2, NP))]
    if qkv:
        scratch += [dma((2,)), dma((NR,)), dma((NR,)), dma((NR,)), dma((NR,)), dma((3,)), dma((3,))]
    return pl.pallas_call(
        functools.partial(_gather_dot, qkv),
        out_shape=out_shape,
        in_specs=[hbm, hbm, hbm],
        out_specs=out_specs,
        scratch_shapes=scratch,
        compiler_params=pltpu.CompilerParams(collective_id=0 if qkv else 1, has_side_effects=True, vmem_limit_bytes=60 * MIB),
        cost_estimate=pl.CostEstimate(flops=2 * R * NT * C * N, bytes_accessed=2 * NT * (R * C + C * N), transcendentals=0),
        name="qkv_dot" if qkv else "out_dot",
    )(x, w, seg)


def _out_dot(x_hbm, w_hbm, y_hbm, xg, wg, wg2, y1, y2, loc, w_send, w_recv, o_send, o_recv, e_send, e_recv, y_send, y_recv):
    R, C = x_hbm.shape
    N = w_hbm.shape[1]
    RC, NH = R // NR, N // (2 * NP)
    d, t, s = lax.axis_index("dp"), lax.axis_index("tp"), lax.axis_index("sp")
    yc, c = s // 2, s % 2
    sib, ynb, diag = s + 1 - 2 * c, s + 2 - 4 * yc, (2 - 2 * yc) + (1 - c)
    mesh_id = pl.DeviceIdType.MESH
    to_sib, to_y, to_x = (d, t, sib), (d, t, ynb), (1 - d, t, s)
    is_end = (t == 0) | (t == NT - 1)
    bar = pltpu.get_barrier_semaphore()

    def greet(who):
        pl.semaphore_signal(bar, inc=1, device_id=who, device_id_type=mesh_id)

    def remote(src, dst, send, recv, who):
        return pltpu.make_async_remote_copy(src, dst, send, recv, device_id=who, device_id_type=mesh_id)

    def rows(r):
        return pl.ds(_mo(r, RC), RC)

    def mine(p):
        return pl.ds(_mo(2 * p + d, NH), NH)

    def other(p):
        return pl.ds(_mo(2 * p + 1 - d, NH), NH)

    kinds = {
        "y2": (wg2, s, mine, to_y, ynb, mine),
        "xo2": (wg2, s, mine, to_x, s, other),
        "so2": (wg2, s, mine, to_sib, sib, mine),
        "x2": (wg2, ynb, mine, to_x, ynb, other),
        "sy2": (wg2, ynb, mine, to_sib, diag, mine),
        "sx2": (wg2, s, other, to_sib, sib, other),
        "sxy2": (wg2, ynb, other, to_sib, diag, other),
        "y1": (wg, s, mine, to_y, ynb, mine),
        "x1": (wg, ynb, mine, to_x, ynb, other),
        "sy1": (wg, ynb, mine, to_sib, diag, mine),
        "sx1": (wg, ynb, other, to_sib, diag, other),
    }
    number = {kind: i for i, kind in enumerate(kinds)}

    def w_out(kind, p):
        panel, owner, cols, who, _, _ = kinds[kind]
        n = number[kind]
        src = w_hbm.at[:, cols(p)] if kind == "y1" else panel.at[owner, :, cols(p)]
        return remote(src, panel.at[owner, :, cols(p)], w_send.at[n, p], w_recv.at[n, p], who)

    def w_in(kind, p):
        panel, _, _, who, owner, cols = kinds[kind]
        n = number[kind]
        at = panel.at[owner, :, cols(p)]
        return remote(at, at, w_send.at[n, p], w_recv.at[n, p], who)

    @pl.when(is_end)
    def _():
        m = (t + 3) // 3
        to_m = (d, m, s)
        greet(to_m)
        pl.semaphore_wait(bar, 1)

        def w_z(p):
            return remote(w_hbm.at[:, mine(p)], wg2.at[s, :, mine(p)], e_send.at[0, p], e_recv.at[0, p], to_m)

        def x_z(r):
            return remote(x_hbm.at[rows(r)], xg.at[t, rows(r)], e_send.at[1, r], e_recv.at[1, r], to_m)

        for p in range(NP):
            w_z(p).start()
        for r in range(NR):
            x_z(r).start()
        for p in range(NP):
            w_z(p).wait_send()
        for r in range(NR):
            x_z(r).wait_send()
        for r in range(NR):
            remote(y_hbm.at[rows(r)], y_hbm.at[rows(r)], y_send.at[r], y_recv.at[r], to_m).wait_recv()

    @pl.when(jnp.logical_not(is_end))
    def _():
        e, o = 3 * t - 3, 3 - t
        oe = 3 - e
        to_e, to_o = (d, e, s), (d, o, s)
        for who in (to_e, to_o, to_y, to_x, to_sib):
            greet(who)
        pl.semaphore_wait(bar, 5)

        def x_own(r):
            return remote(x_hbm.at[rows(r)], xg.at[t, rows(r)], o_send.at[0, r], o_recv.at[0, r], to_o)

        def x_end(r):
            return remote(xg.at[e, rows(r)], xg.at[e, rows(r)], o_send.at[1, r], o_recv.at[1, r], to_o)

        def x_in(i, r):
            k = o if i == 0 else oe
            return remote(xg.at[k, rows(r)], xg.at[k, rows(r)], o_send.at[i, r], o_recv.at[i, r], to_o)

        def relay_end(r):
            remote(xg.at[e, rows(r)], xg.at[e, rows(r)], e_send.at[1, r], e_recv.at[1, r], to_e).wait_recv()
            x_end(r).start()

        own_x = pltpu.make_async_copy(x_hbm, xg.at[t], loc.at[0])
        own_w = pltpu.make_async_copy(w_hbm, wg.at[s], loc.at[1])
        w_so1 = remote(w_hbm, wg.at[s], loc.at[2], loc.at[3], to_sib)
        w_so1_in = remote(w_hbm, wg.at[sib], loc.at[2], loc.at[3], to_sib)
        for r in range(NR):
            x_own(r).start()
        own_x.start()
        own_w.start()
        w_so1.start()

        for i in range(NR + NP):
            if i < NP:
                at = wg2.at[s, :, mine(i)]
                remote(at, at, e_send.at[0, i], e_recv.at[0, i], to_e).wait_recv()
                w_out("y2", i).start()
                w_out("xo2", i).start()
                w_out("so2", i).start()
            if i == NP - 1:
                for p in range(NP):
                    w_out("y1", p).start()
            if 1 <= i <= NP:
                w_in("y2", i - 1).wait_recv()
                w_out("x2", i - 1).start()
                w_out("sy2", i - 1).start()
            if i >= NP:
                relay_end(i - NP)
                if i < 2 * NP:
                    w_in("y1", i - NP).wait_recv()
                    w_out("x1", i - NP).start()
                    w_out("sy1", i - NP).start()
                    w_in("xo2", i - NP).wait_recv()
                    w_out("sx2", i - NP).start()
                else:
                    w_in("x2", i - 2 * NP).wait_recv()
                    w_out("sxy2", i - 2 * NP).start()
        for kind in ("so2", "sy2", "sx2", "sxy2"):
            for p in range(NP):
                w_in(kind, p).wait_recv()
        own_x.wait()

        def unit(panel, out, r):
            acc = jnp.dot(xg[0, rows(r), :], panel[0], preferred_element_type=jnp.float32)
            for k in range(1, NT):
                acc += jnp.dot(xg[k, rows(r), :], panel[k], preferred_element_type=jnp.float32)
            out[rows(r), :] = acc.astype(jnp.bfloat16)

        def y_out(r):
            return remote(y2.at[rows(r)], y_hbm.at[rows(r)], y_send.at[r], y_recv.at[r], to_e)

        def first(r, z):
            x_in(0, r).wait_recv()
            x_in(1, r).wait_recv()
            unit(wg2, y2, r)

            @pl.when(r > 0)
            def _():
                y_out(r - 1).start()

            return z

        half = NR // 2
        lax.fori_loop(0, half, first, 0)
        y_out(half - 1).start()
        for p in range(NP):
            w_in("x1", p).wait_recv()
            w_out("sx1", p).start()
        own_w.wait()
        w_so1_in.wait_recv()
        for kind in ("sy1", "sx1"):
            for p in range(NP):
                w_in(kind, p).wait_recv()

        def second(r, z):
            x_in(0, r).wait_recv()
            x_in(1, r).wait_recv()
            unit(wg2, y2, r)

            def own(i, z):
                unit(wg, y1, 2 * (r - half) + i)

                @pl.when(i == 0)
                def _():
                    y_out(r).start()

                return z

            return lax.fori_loop(0, 2, own, z)

        lax.fori_loop(half, NR, second, 0)
        own_y = pltpu.make_async_copy(y1, y_hbm, loc.at[0])
        own_y.start()
        w_so1.wait_send()
        for r in range(NR):
            x_own(r).wait_send()
            x_end(r).wait_send()
            y_out(r).wait_send()
        for kind in kinds:
            for p in range(NP):
                w_out(kind, p).wait_send()
        own_y.wait()


def _out_call(x, w):
    R, C = x.shape
    N = w.shape[1]
    dma = pltpu.SemaphoreType.DMA
    hbm = pl.BlockSpec(memory_space=pltpu.HBM)
    bf16 = jnp.bfloat16
    return pl.pallas_call(
        _out_dot,
        out_shape=jax.ShapeDtypeStruct((R, N), bf16),
        in_specs=[hbm, hbm],
        out_specs=hbm,
        scratch_shapes=[
            pltpu.VMEM((NT, R, C), bf16),
            pltpu.VMEM((NT, C, N), bf16),
            pltpu.VMEM((NT, C, N), bf16),
            pltpu.VMEM((R, N), bf16),
            pltpu.VMEM((R, N), bf16),
            dma((4,)), dma((11, NP)), dma((11, NP)), dma((2, NR)), dma((2, NR)), dma((2, NR)), dma((2, NR)), dma((NR,)), dma((NR,)),
        ],
        compiler_params=pltpu.CompilerParams(collective_id=1, has_side_effects=True, vmem_limit_bytes=60 * MIB),
        cost_estimate=pl.CostEstimate(flops=4 * R * NT * C * N, bytes_accessed=2 * NT * (R * C + C * N), transcendentals=0),
        name="out_dot",
    )(x, w)


def _attention(BQ, BK, s_ref, seg_ref, q_ref, kv_ref, o_ref, st_ref, sc_ref, m_ref, l_ref, acc_ref):
    R = q_ref.shape[0]
    s = s_ref[0]
    seg = seg_ref[...]
    scale = LOG2E / HEAD_DIM ** 0.5
    for doc in range(1, 4):
        st_ref[doc] = jnp.sum((seg < doc).astype(jnp.int32))

    def doc_start(row):
        out = jnp.zeros_like(row)
        for doc in range(1, 4):
            start = st_ref[doc]
            out = jnp.where(start <= row, jnp.maximum(out, start), out)
        return out

    def lane_groups(a, op):
        out = a[:, :HEAD_DIM]
        for g in range(1, a.shape[1] // HEAD_DIM):
            out = op(out, a[:, HEAD_DIM * g : HEAD_DIM * (g + 1)])
        return out

    def q_block(b, z):
        row0 = s * R + b * BQ
        q_at = pl.ds(_mo(b, BQ), BQ)
        lo = doc_start(row0) // BK
        hi = (row0 + BQ - 1) // BK + 1
        full_lo = jnp.clip((doc_start(row0 + BQ - 1) + BK - 1) // BK, lo, hi)
        full_hi = jnp.clip((row0 + 1) // BK, full_lo, hi)
        m_ref[...] = jnp.full(m_ref.shape, -3e38, jnp.float32)
        l_ref[...] = jnp.zeros(l_ref.shape, jnp.float32)
        acc_ref[...] = jnp.zeros(acc_ref.shape, jnp.float32)

        def scores(j, z, masked):
            k_at = pl.ds(_mo(j, BK), BK)
            if masked:
                row_id = row0 + lax.broadcasted_iota(jnp.int32, (BQ, 1), 0)
                key_id = j * BK + lax.broadcasted_iota(jnp.int32, (BQ, BK), 1)
                seen = (key_id <= row_id) & (key_id >= doc_start(row_id))
            for h in range(2):
                q = q_ref[q_at, HEAD_DIM * h : HEAD_DIM * (h + 1)]
                k = kv_ref[k_at, 2 * HEAD_DIM * h : 2 * HEAD_DIM * h + HEAD_DIM]
                sc = lax.dot_general(q, k, (((1,), (1,)), ((), ())), preferred_element_type=jnp.float32)
                if masked:
                    sc = jnp.where(seen, sc, -jnp.inf)
                sc_ref[h, j] = sc
                m_ref[h] = jnp.maximum(m_ref[h], lane_groups(sc, jnp.maximum))
            return z

        def weights(j, z):
            for h in range(2):
                m = m_ref[h]
                e = jnp.exp2((sc_ref[h, j] - jnp.concatenate([m] * (BK // HEAD_DIM), axis=1)) * scale)
                sc_ref[h, j] = e
                l_ref[h] = l_ref[h] + lane_groups(e, jnp.add)
            return z

        def values(j, z):
            k_at = pl.ds(_mo(j, BK), BK)
            for h in range(2):
                v = kv_ref[k_at, 2 * HEAD_DIM * h + HEAD_DIM : 2 * HEAD_DIM * (h + 1)]
                p = (sc_ref[h, j] * jnp.concatenate([l_ref[h]] * (BK // HEAD_DIM), axis=1)).astype(jnp.bfloat16)
                acc_ref[h] = acc_ref[h] + jnp.dot(p, v, preferred_element_type=jnp.float32)
            return z

        lax.fori_loop(lo, full_lo, functools.partial(scores, masked=True), 0)
        lax.fori_loop(full_lo, full_hi, functools.partial(scores, masked=False), 0)
        lax.fori_loop(full_hi, hi, functools.partial(scores, masked=True), 0)
        for h in range(2):
            m_ref[h] = jnp.broadcast_to(jnp.max(m_ref[h], axis=1, keepdims=True), (BQ, HEAD_DIM))
        lax.fori_loop(lo, hi, weights, 0)
        for h in range(2):
            l_ref[h] = jnp.broadcast_to(1.0 / jnp.sum(l_ref[h], axis=1, keepdims=True), (BQ, HEAD_DIM))
        lax.fori_loop(lo, hi, values, 0)
        for h in range(2):
            o_ref[q_at, HEAD_DIM * h : HEAD_DIM * (h + 1)] = acc_ref[h].astype(jnp.bfloat16)
        return z

    lax.fori_loop(0, R // BQ, q_block, 0)


def _attention_call(q, kv_all, seg_all):
    R, cols = q.shape
    rows = NT * R
    BQ, BK = min(512, R), min(512, R)
    s = lax.axis_index("sp").astype(jnp.int32).reshape(1)
    return pl.pallas_call(
        functools.partial(_attention, BQ, BK),
        out_shape=jax.ShapeDtypeStruct((R, cols), jnp.bfloat16),
        grid_spec=pltpu.PrefetchScalarGridSpec(
            num_scalar_prefetch=1,
            grid=(cols // (2 * HEAD_DIM),),
            in_specs=[
                pl.BlockSpec(seg_all.shape, lambda p, s: (0, 0)),
                pl.BlockSpec((R, 2 * HEAD_DIM), lambda p, s: (0, p)),
                pl.BlockSpec((rows, 4 * HEAD_DIM), lambda p, s: (0, p)),
            ],
            out_specs=pl.BlockSpec((R, 2 * HEAD_DIM), lambda p, s: (0, p)),
            scratch_shapes=[
                pltpu.SMEM((4,), jnp.int32),
                pltpu.VMEM((2, rows // BK, BQ, BK), jnp.float32),
                pltpu.VMEM((2, BQ, HEAD_DIM), jnp.float32),
                pltpu.VMEM((2, BQ, HEAD_DIM), jnp.float32),
                pltpu.VMEM((2, BQ, HEAD_DIM), jnp.float32),
            ],
        ),
        compiler_params=pltpu.CompilerParams(vmem_limit_bytes=48 * MIB),
        cost_estimate=pl.CostEstimate(flops=2 * R * rows * cols, bytes_accessed=4 * rows * cols, transcendentals=R * rows * cols // 256),
        name="attention",
    )(s, seg_all, q, kv_all)


def solution(mesh):
    def local_block(x_blk, wqkv_blk, wout_blk, seg_blk):
        R = x_blk.shape[0]
        seg = seg_blk.reshape(-1, 128)
        q, kv_all, seg_all = _gather_call(True, x_blk, wqkv_blk, seg)
        context = _attention_call(q, kv_all.reshape(NT * R, -1), seg_all.reshape(-1, 128))
        return _out_call(context, wout_blk)

    row_spec = P(("dp", "sp"), "tp")
    return jax.shard_map(local_block, mesh=mesh, in_specs=(row_spec, P("sp", "tp"), P("sp", "tp"), P(("dp", "sp"))), out_specs=row_spec, check_vma=False)
```

```python
import functools

import jax
import jax.numpy as jnp
from jax import lax
from jax.experimental import pallas as pl
from jax.experimental.pallas import tpu as pltpu
from jax.sharding import PartitionSpec as P

HEAD_DIM = 128
NT = 4
NR = 8
NB = 4
NP = 4
LOG2E = 1.4426950408889634
MIB = 1024 * 1024


def _mo(i, n):
    return pl.multiple_of(i * n, n)


def _gather_dot(qkv, x_hbm, w_hbm, seg_hbm, *refs):
    if qkv:
        q_ref, kv_all, seg_all = refs[:3]
        refs = refs[3:]
    else:
        (y_ref,) = refs[:1]
        refs = refs[1:]
    xg, wg = refs[:2]
    refs = refs[2:]
    if qkv:
        kv = refs[0]
        refs = refs[1:]
    loc, xs, xl, xr, ws_own, ws_y, ws_x, ws_f, wr_own, wr_y, wr_x, wr_f = refs[:12]
    if qkv:
        kv_send, kv_yr, kv_cr, kv_fs, kv_fr, seg_s, seg_r = refs[12:]

    R, C = x_hbm.shape
    N = w_hbm.shape[1]
    RC, NG, NH = R // NR, N // NP, N // (2 * NP)
    d, t, s = lax.axis_index("dp"), lax.axis_index("tp"), lax.axis_index("sp")
    yc, c = s // 2, s % 2
    sib, ynb, diag = s + 1 - 2 * c, s + 2 - 4 * yc, (2 - 2 * yc) + (1 - c)
    mesh_id = pl.DeviceIdType.MESH
    to_sib, to_y, to_diag = (d, t, sib), (d, t, ynb), (d, t, diag)
    to_x = (1 - d, t, s)
    to_right, to_left = (d, t + 1, s), (d, t - 1, s)
    has_right, has_left = t < NT - 1, t > 0

    bar = pltpu.get_barrier_semaphore()

    def greet(who):
        pl.semaphore_signal(bar, inc=1, device_id=who, device_id_type=mesh_id)

    greet(to_sib)
    greet(to_y)
    greet(to_x)
    if qkv:
        greet(to_diag)

    @pl.when(has_right)
    def _():
        greet(to_right)

    @pl.when(has_left)
    def _():
        greet(to_left)

    base = 4 if qkv else 3

    @pl.when(has_right & has_left)
    def _():
        pl.semaphore_wait(bar, base + 2)

    @pl.when(jnp.logical_not(has_right & has_left))
    def _():
        pl.semaphore_wait(bar, base + 1)

    def remote(src, dst, send, recv, who):
        return pltpu.make_async_remote_copy(src, dst, send, recv, device_id=who, device_id_type=mesh_id)

    def w_own(p):
        cols = pl.ds(p * NG, NG)
        return remote(w_hbm.at[:, cols], wg.at[s, :, cols], ws_own.at[p], wr_own.at[p], to_sib)

    def w_own_in(p):
        cols = pl.ds(p * NG, NG)
        return remote(w_hbm.at[:, cols], wg.at[sib, :, cols], ws_own.at[p], wr_own.at[p], to_sib)

    def mine(p):
        return pl.ds(_mo(2 * p + d, NH), NH)

    def other(p):
        return pl.ds(_mo(2 * p + 1 - d, NH), NH)

    def w_y(p):
        return remote(w_hbm.at[:, mine(p)], wg.at[s, :, mine(p)], ws_y.at[p], wr_y.at[p], to_y)

    def w_y_in(p):
        return remote(w_hbm.at[:, mine(p)], wg.at[ynb, :, mine(p)], ws_y.at[p], wr_y.at[p], to_y)

    def w_x(p):
        return remote(wg.at[ynb, :, mine(p)], wg.at[ynb, :, mine(p)], ws_x.at[p], wr_x.at[p], to_x)

    def w_x_in(p):
        return remote(wg.at[ynb, :, other(p)], wg.at[ynb, :, other(p)], ws_x.at[p], wr_x.at[p], to_x)

    def w_f(p, which):
        cols = mine(p) if which == 0 else other(p)
        return remote(wg.at[ynb, :, cols], wg.at[ynb, :, cols], ws_f.at[which, p], wr_f.at[which, p], to_sib)

    def w_f_in(p, which):
        cols = mine(p) if which == 0 else other(p)
        return remote(wg.at[diag, :, cols], wg.at[diag, :, cols], ws_f.at[which, p], wr_f.at[which, p], to_sib)

    def rows(r):
        return pl.ds(_mo(r, RC), RC)

    def x_own(r, way):
        recv = xl if way == 0 else xr
        return remote(x_hbm.at[rows(r)], xg.at[t, rows(r)], xs.at[way, 0, r], recv.at[0, r], to_right if way == 0 else to_left)

    def x_arrive(r, way, dist):
        k = t - dist if way == 0 else t + dist
        recv = xl if way == 0 else xr
        return remote(xg.at[k, rows(r)], xg.at[k, rows(r)], xs.at[way, 0, r], recv.at[dist - 1, r], to_right if way == 0 else to_left)

    def x_forward(r, way, dist):
        k = t - dist if way == 0 else t + dist
        recv = xl if way == 0 else xr
        return remote(xg.at[k, rows(r)], xg.at[k, rows(r)], xs.at[way, dist, r], recv.at[dist, r], to_right if way == 0 else to_left)

    def send_own_x(r):
        @pl.when(has_right)
        def _():
            x_own(r, 0).start()

        @pl.when(has_left)
        def _():
            x_own(r, 1).start()

    def relay_x(r):
        for dist in range(1, NT):
            for way in range(2):
                here = (t >= dist) if way == 0 else (t <= NT - 1 - dist)

                @pl.when(here)
                def _():
                    x_arrive(r, way, dist).wait_recv()
                    if dist < NT - 1:
                        @pl.when(has_right if way == 0 else has_left)
                        def _():
                            x_forward(r, way, dist).start()

    own_x = pltpu.make_async_copy(x_hbm, xg.at[t], loc.at[0])
    own_w = pltpu.make_async_copy(w_hbm, wg.at[s], loc.at[1])
    for r in range(2):
        send_own_x(r)
    for p in range(NP):
        w_y(p).start()
    for p in range(NP):
        w_own(p).start()
    own_x.start()
    own_w.start()
    if qkv:
        own_seg = pltpu.make_async_copy(seg_hbm, seg_all.at[s], loc.at[3])
        own_seg.start()
        peers = ((to_sib, sib), (to_y, ynb), (to_diag, diag))

        def seg_out(i):
            return remote(seg_hbm, seg_all.at[s], seg_s.at[i], seg_r.at[i], peers[i][0])

        def seg_in(i):
            return remote(seg_hbm, seg_all.at[peers[i][1]], seg_s.at[i], seg_r.at[i], peers[i][0])

        for i in range(3):
            seg_out(i).start()

    def unit(r, p):
        cols = pl.ds(_mo(p, NG), NG)
        acc = jnp.dot(xg[0, rows(r), :], wg[0, :, cols], preferred_element_type=jnp.float32)
        for k in range(1, NT):
            acc += jnp.dot(xg[k, rows(r), :], wg[k, :, cols], preferred_element_type=jnp.float32)
        out = acc.astype(jnp.bfloat16)
        if qkv:
            for h in range(2):
                at = 3 * HEAD_DIM * h
                q_ref[rows(r), pl.ds(pl.multiple_of(p * (2 * HEAD_DIM) + h * HEAD_DIM, HEAD_DIM), HEAD_DIM)] = out[:, at : at + HEAD_DIM]
                kv[rows(r), pl.ds(_mo(2 * p + h, 2 * HEAD_DIM), 2 * HEAD_DIM)] = out[:, at + HEAD_DIM : at + 3 * HEAD_DIM]
        else:
            y_ref[rows(r), cols] = out

    def kv_cols(p):
        return pl.ds(_mo(p, 4 * HEAD_DIM), 4 * HEAD_DIM)

    def kv_unit(r, p, who, send, recv):
        return remote(kv.at[rows(r), kv_cols(p)], kv_all.at[s, rows(r), kv_cols(p)], send, recv, who)

    def send_unit(r, p):
        pltpu.make_async_copy(kv.at[rows(r), kv_cols(p)], kv_all.at[s, rows(r), kv_cols(p)], loc.at[2]).start()

        @pl.when(yc == 0)
        def _():
            kv_unit(r, p, to_y, kv_send.at[0], kv_yr.at[r]).start()

        @pl.when(c == 0)
        def _():
            kv_unit(r, p, to_sib, kv_send.at[1], kv_cr.at[r]).start()

    def do_units(work):
        for n, f in work:
            def body(u, z, f=f):
                unit(*f(u))
                return z
            lax.fori_loop(0, n, body, 0)
        if qkv:
            for n, f in work:
                def body(u, z, f=f):
                    send_unit(*f(u))
                    return z
                lax.fori_loop(0, n, body, 0)

    def kv_row(r, owner, who, send, recv):
        return remote(kv_all.at[owner, rows(r)], kv_all.at[owner, rows(r)], send, recv, who)

    def pass_kv(r):
        if qkv:
            @pl.when(yc == 1)
            def _():
                kv_row(r, ynb, to_y, kv_fs.at[r], kv_yr.at[r]).wait_recv()
                kv_row(r, ynb, to_sib, kv_fs.at[r], kv_fr.at[r]).start()

    def relay_w(i):
        if i < NP:
            w_y_in(i).wait_recv()
            w_x(i).start()
            w_f(i, 0).start()
        if 1 <= i <= NP:
            w_x_in(i - 1).wait_recv()
            w_f(i - 1, 1).start()
            p = i - 1
            if p == 0:
                own_x.wait()
                own_w.wait()
            w_own_in(p).wait_recv()
            w_f_in(p, 0).wait_recv()
            w_f_in(p, 1).wait_recv()

    for i in range(NP + 1):
        relay_x(i)
        send_own_x(i + 2)
        relay_w(i)
        if i == 2:
            do_units([(6, lambda u: (u // 2, u % 2))])
        if i == 3:
            do_units([(2, lambda u: (3, u)), (4, lambda u: (u, 2))])
        if i == 4:
            do_units([(3, lambda u: (4, u)), (5, lambda u: (u, 3))])

    def late(i, z):
        relay_x(i)

        @pl.when(i + 2 < NR)
        def _():
            send_own_x(i + 2)

        pass_kv(2 * (i - NP - 1))
        pass_kv(2 * (i - NP - 1) + 1)
        do_units([(NP, lambda u: (i, u))])
        return z

    lax.fori_loop(NP + 1, NR, late, 0)

    for p in range(NP):
        w_own(p).wait_send()
        w_y(p).wait_send()
        w_x(p).wait_send()
        w_f(p, 0).wait_send()
        w_f(p, 1).wait_send()

    def drain_x(r, z):
        @pl.when(has_right)
        def _():
            x_own(r, 0).wait_send()
            for dist in range(1, NT - 1):
                @pl.when(t >= dist)
                def _():
                    x_forward(r, 0, dist).wait_send()

        @pl.when(has_left)
        def _():
            x_own(r, 1).wait_send()
            for dist in range(1, NT - 1):
                @pl.when(t <= NT - 1 - dist)
                def _():
                    x_forward(r, 1, dist).wait_send()

        return z

    lax.fori_loop(0, NR, drain_x, 0)
    if qkv:
        pass_kv(6)
        pass_kv(7)
        own_seg.wait()
        for i in range(3):
            seg_out(i).wait_send()
            seg_in(i).wait_recv()
        pltpu.make_async_copy(kv, kv_all.at[s], loc.at[2]).wait()

        @pl.when(yc == 0)
        def _():
            remote(kv, kv_all.at[s], kv_send.at[0], kv_yr.at[0], to_y).wait_send()

        @pl.when(c == 0)
        def _():
            remote(kv, kv_all.at[s], kv_send.at[1], kv_cr.at[0], to_sib).wait_send()

        def drain_kv(r, z):
            @pl.when(c == 1)
            def _():
                kv_row(r, sib, to_sib, kv_fs.at[r], kv_cr.at[r]).wait_recv()

            @pl.when(yc == 1)
            def _():
                kv_row(r, ynb, to_sib, kv_fs.at[r], kv_fr.at[r]).wait_send()
                kv_row(r, diag, to_sib, kv_fs.at[r], kv_fr.at[r]).wait_recv()

            return z

        lax.fori_loop(0, NR, drain_kv, 0)


def _gather_call(qkv, x, w, seg):
    R, C = x.shape
    N = w.shape[1]
    dma = pltpu.SemaphoreType.DMA
    hbm = pl.BlockSpec(memory_space=pltpu.HBM)
    vmem = pl.BlockSpec(memory_space=pltpu.VMEM)
    bf16 = jnp.bfloat16
    scratch = [pltpu.VMEM((NT, R, C), bf16), pltpu.VMEM((NT, C, N), bf16)]
    if qkv:
        heads = N // (3 * HEAD_DIM)
        out_shape = (
            jax.ShapeDtypeStruct((R, heads * HEAD_DIM), bf16),
            jax.ShapeDtypeStruct((NT, R, 2 * heads * HEAD_DIM), bf16),
            jax.ShapeDtypeStruct((NT,) + seg.shape, jnp.int32),
        )
        out_specs = (vmem, hbm, hbm)
        scratch.append(pltpu.VMEM((R, 2 * heads * HEAD_DIM), bf16))
    else:
        out_shape = jax.ShapeDtypeStruct((R, N), bf16)
        out_specs = vmem
    scratch += [dma((4,)), dma((2, 3, NR)), dma((3, NR)), dma((3, NR)), dma((NP,)), dma((NP,)), dma((NP,)), dma((2, NP)),
                dma((NP,)), dma((NP,)), dma((NP,)), dma((2, NP))]
    if qkv:
        scratch += [dma((2,)), dma((NR,)), dma((NR,)), dma((NR,)), dma((NR,)), dma((3,)), dma((3,))]
    return pl.pallas_call(
        functools.partial(_gather_dot, qkv),
        out_shape=out_shape,
        in_specs=[hbm, hbm, hbm],
        out_specs=out_specs,
        scratch_shapes=scratch,
        compiler_params=pltpu.CompilerParams(collective_id=0 if qkv else 1, has_side_effects=True, vmem_limit_bytes=60 * MIB),
        cost_estimate=pl.CostEstimate(flops=2 * R * NT * C * N, bytes_accessed=2 * NT * (R * C + C * N), transcendentals=0),
        name="qkv_dot" if qkv else "out_dot",
    )(x, w, seg)


def _attend_out(q_hbm, kv_hbm, seg_hbm, w_hbm, y_hbm, q_ref, kv_ref, seg_ref, first_ref, sc_ref, m_ref, l_ref, acc_ref, xg, wg, wg2, y1, y2,
                loc, kv_sem, w_send, w_recv, o_send, o_recv, e_send, e_recv, z_send, z_recv, y_send, y_recv):
    R, C = q_hbm.shape
    N = w_hbm.shape[1]
    RC, NH = R // NR, N // (2 * NP)
    BQ = R // NB
    BK = 2 * BQ
    CP = 2 * HEAD_DIM
    NU = NB * (C // CP)
    d, t, s = lax.axis_index("dp"), lax.axis_index("tp"), lax.axis_index("sp")
    yc, c = s // 2, s % 2
    sib, ynb, diag = s + 1 - 2 * c, s + 2 - 4 * yc, (2 - 2 * yc) + (1 - c)
    mesh_id = pl.DeviceIdType.MESH
    to_sib, to_y, to_x = (d, t, sib), (d, t, ynb), (1 - d, t, s)
    is_end = (t == 0) | (t == NT - 1)
    is_mid = jnp.logical_not(is_end)
    e, o = 3 * t - 3, 3 - t
    oe = 3 - e
    m_plane = (t + 3) // 3
    to_m, to_e, to_o = (d, m_plane, s), (d, e, s), (d, o, s)
    bar = pltpu.get_barrier_semaphore()

    def greet(who):
        pl.semaphore_signal(bar, inc=1, device_id=who, device_id_type=mesh_id)

    def remote(src, dst, send, recv, who):
        return pltpu.make_async_remote_copy(src, dst, send, recv, device_id=who, device_id_type=mesh_id)

    def rows(r):
        return pl.ds(_mo(r, RC), RC)

    def mine(p):
        return pl.ds(_mo(2 * p + d, NH), NH)

    def other(p):
        return pl.ds(_mo(2 * p + 1 - d, NH), NH)

    def piece(k, u):
        return xg.at[k, pl.ds(_mo(u // (C // CP), BQ), BQ), pl.ds(_mo(u % (C // CP), CP), CP)]

    kinds = {
        "y2": (wg2, s, mine, to_y, ynb, mine),
        "xo2": (wg2, s, mine, to_x, s, other),
        "so2": (wg2, s, mine, to_sib, sib, mine),
        "x2": (wg2, ynb, mine, to_x, ynb, other),
        "sy2": (wg2, ynb, mine, to_sib, diag, mine),
        "sx2": (wg2, s, other, to_sib, sib, other),
        "sxy2": (wg2, ynb, other, to_sib, diag, other),
        "y1": (wg, s, mine, to_y, ynb, mine),
        "x1": (wg, ynb, mine, to_x, ynb, other),
        "sy1": (wg, ynb, mine, to_sib, diag, mine),
        "sx1": (wg, ynb, other, to_sib, diag, other),
    }
    number = {kind: i for i, kind in enumerate(kinds)}

    def w_out(kind, p):
        panel, owner, cols, who, _, _ = kinds[kind]
        n = number[kind]
        src = w_hbm.at[:, cols(p)] if kind == "y1" else panel.at[owner, :, cols(p)]
        return remote(src, panel.at[owner, :, cols(p)], w_send.at[n, p], w_recv.at[n, p], who)

    def w_in(kind, p):
        panel, _, _, who, owner, cols = kinds[kind]
        n = number[kind]
        at = panel.at[owner, :, cols(p)]
        return remote(at, at, w_send.at[n, p], w_recv.at[n, p], who)

    def w_z(p, who):
        return remote(w_hbm.at[:, mine(p)], wg2.at[s, :, mine(p)], z_send.at[p], z_recv.at[p], who)

    def end_piece(u, who):
        k = t if who is to_m else e
        return remote(piece(k, u), piece(k, u), e_send.at[u], e_recv.at[u], who)

    def own_piece(u):
        return remote(piece(t, u), piece(t, u), o_send.at[0, u], o_recv.at[0, u], to_o)

    def passed_piece(u):
        return remote(piece(e, u), piece(e, u), o_send.at[1, u], o_recv.at[1, u], to_o)

    def piece_in(i, u):
        k = o if i == 0 else oe
        return remote(piece(k, u), piece(k, u), o_send.at[i, u], o_recv.at[i, u], to_o)

    def y_out(r, who):
        return remote(y2.at[rows(r)], y_hbm.at[rows(r)], y_send.at[r], y_recv.at[r], who)

    q_copy = pltpu.make_async_copy(q_hbm, q_ref, loc.at[0])
    seg_copy = pltpu.make_async_copy(seg_hbm, seg_ref, loc.at[1])
    own_w = pltpu.make_async_copy(w_hbm, wg.at[s], loc.at[2])

    def kv_copy(g, k):
        return pltpu.make_async_copy(kv_hbm.at[k, :, pl.ds(_mo(g, 2 * CP), 2 * CP)], kv_ref.at[g, pl.ds(_mo(k, R), R)], kv_sem.at[g, k])

    w_so1 = remote(w_hbm, wg.at[s], loc.at[3], loc.at[4], to_sib)
    w_so1_in = remote(w_hbm, wg.at[sib], loc.at[3], loc.at[4], to_sib)
    seg_copy.start()
    q_copy.start()
    for g in range(C // CP):
        for k in range(NT):
            @pl.when(k <= s)
            def _():
                kv_copy(g, k).start()

    @pl.when(is_end)
    def _():
        greet(to_m)
        pl.semaphore_wait(bar, 1)
        for p in range(NP):
            w_z(p, to_m).start()

    @pl.when(is_mid)
    def _():
        for who in (to_e, to_o, to_y, to_x, to_sib):
            greet(who)
        pl.semaphore_wait(bar, 5)
        own_w.start()
        w_so1.start()

    seg_copy.wait()
    seg = seg_ref[...]
    starts = [jnp.sum(jnp.where(seg < doc, 1.0, 0.0), axis=(0, 1), keepdims=True) for doc in range(1, 4)]

    def first_rows(b, z):
        row = (s * R + b * BQ + lax.broadcasted_iota(jnp.int32, (BQ, HEAD_DIM), 0)).astype(jnp.float32)
        out = jnp.zeros((BQ, HEAD_DIM), jnp.float32)
        for start in starts:
            out = jnp.where(start <= row, jnp.maximum(out, start), out)
        first_ref[pl.ds(_mo(b, BQ), BQ), :] = out.astype(jnp.int32)
        return z

    lax.fori_loop(0, NB, first_rows, 0)
    q_copy.wait()

    scale = LOG2E / HEAD_DIM ** 0.5

    def lane_groups(a, op):
        out = a[:, :HEAD_DIM]
        for g in range(1, a.shape[1] // HEAD_DIM):
            out = op(out, a[:, HEAD_DIM * g : HEAD_DIM * (g + 1)])
        return out

    def wide(a):
        return jnp.concatenate([a] * (BK // HEAD_DIM), axis=1)

    def attend(u):
        b, g = u // (C // CP), u % (C // CP)
        q_at = pl.ds(_mo(b, BQ), BQ)
        full = (s * R) // BK + b // 2
        m_ref[...] = jnp.full(m_ref.shape, -3e38, jnp.float32)
        l_ref[...] = jnp.zeros(l_ref.shape, jnp.float32)
        acc_ref[...] = jnp.zeros(acc_ref.shape, jnp.float32)

        def scores(j, z, diagonal):
            k_at = pl.ds(_mo(j, BK), BK)
            key_id = j * BK + lax.broadcasted_iota(jnp.int32, (BQ, BK), 1)
            seen = key_id >= wide(first_ref[q_at, :])
            if diagonal:
                seen = seen & (key_id <= s * R + b * BQ + lax.broadcasted_iota(jnp.int32, (BQ, BK), 0))
            for h in range(2):
                q = q_ref[q_at, pl.ds(pl.multiple_of(g * CP + h * HEAD_DIM, HEAD_DIM), HEAD_DIM)]
                k = kv_ref[g, k_at, 2 * HEAD_DIM * h : 2 * HEAD_DIM * h + HEAD_DIM]
                sc = lax.dot_general(q, k, (((1,), (1,)), ((), ())), preferred_element_type=jnp.float32)
                sc = jnp.where(seen, sc, -jnp.inf)
                sc_ref[h, j] = sc
                m_ref[h] = jnp.maximum(m_ref[h], lane_groups(sc, jnp.maximum))
            return z

        def weights(j, z):
            for h in range(2):
                p = jnp.exp2((sc_ref[h, j] - wide(m_ref[h])) * scale)
                sc_ref[h, j] = p
                l_ref[h] = l_ref[h] + lane_groups(p, jnp.add)
            return z

        def values(j, z):
            k_at = pl.ds(_mo(j, BK), BK)
            for h in range(2):
                v = kv_ref[g, k_at, 2 * HEAD_DIM * h + HEAD_DIM : 2 * HEAD_DIM * (h + 1)]
                p = (sc_ref[h, j] * wide(l_ref[h])).astype(jnp.bfloat16)
                acc_ref[h] = acc_ref[h] + jnp.dot(p, v, preferred_element_type=jnp.float32)
            return z

        lax.fori_loop(0, full, functools.partial(scores, diagonal=False), 0)
        scores(full, 0, True)
        for h in range(2):
            m_ref[h] = jnp.broadcast_to(jnp.max(m_ref[h], axis=1, keepdims=True), (BQ, HEAD_DIM))
        lax.fori_loop(0, full + 1, weights, 0)
        for h in range(2):
            l_ref[h] = jnp.broadcast_to(1.0 / jnp.sum(l_ref[h], axis=1, keepdims=True), (BQ, HEAD_DIM))
        lax.fori_loop(0, full + 1, values, 0)
        for h in range(2):
            xg[t, q_at, pl.ds(pl.multiple_of(g * CP + h * HEAD_DIM, HEAD_DIM), HEAD_DIM)] = acc_ref[h].astype(jnp.bfloat16)

    def dot_rows(panel, out, r):
        acc = jnp.dot(xg[0, rows(r), :], panel[0], preferred_element_type=jnp.float32)
        for k in range(1, NT):
            acc += jnp.dot(xg[k, rows(r), :], panel[k], preferred_element_type=jnp.float32)
        out[rows(r), :] = acc.astype(jnp.bfloat16)

    def project(lo, hi):
        def chunk(r, z):
            dot_rows(wg2, y2, r)
            dot_rows(wg, y1, r)
            y_out(r, to_e).start()
            return z

        lax.fori_loop(lo, hi, chunk, 0)

    def pieces_in(lo, hi):
        def wait(u, z):
            piece_in(0, u).wait_recv()
            piece_in(1, u).wait_recv()
            return z

        lax.fori_loop(lo, hi, wait, 0)

    def relay_piece(u):
        end_piece(u, to_e).wait_recv()
        passed_piece(u).start()

    def relay_w(u):
        @pl.when(u < NP)
        def _():
            w_z(u, to_e).wait_recv()
            w_out("y2", u).start()
            w_out("xo2", u).start()
            w_out("so2", u).start()

        @pl.when(u == NP - 1)
        def _():
            for p in range(NP):
                w_out("y1", p).start()

        @pl.when((u >= 1) & (u <= NP))
        def _():
            w_in("y2", u - 1).wait_recv()
            w_out("x2", u - 1).start()
            w_out("sy2", u - 1).start()

        @pl.when((u >= NP) & (u < 2 * NP))
        def _():
            p = u - NP
            w_in("y1", p).wait_recv()
            w_out("x1", p).start()
            w_out("sy1", p).start()
            w_in("xo2", p).wait_recv()
            w_out("sx2", p).start()

        @pl.when((u >= 2 * NP) & (u < 3 * NP))
        def _():
            p = u - 2 * NP
            w_in("x2", p).wait_recv()
            w_out("sxy2", p).start()
            w_in("x1", p).wait_recv()
            w_out("sx1", p).start()

        @pl.when(u == 3 * NP - 1)
        def _():
            own_w.wait()
            w_so1_in.wait_recv()
            for kind in ("so2", "sy2", "sx2", "sxy2", "sy1", "sx1"):
                for p in range(NP):
                    w_in(kind, p).wait_recv()

    per = C // CP
    cb = BQ // RC

    def step(u, z):
        @pl.when(u < per)
        def _():
            for k in range(NT):
                @pl.when(k <= s)
                def _():
                    kv_copy(u, k).wait()

        attend(u)

        @pl.when(is_end)
        def _():
            end_piece(u, to_m).start()

        @pl.when(is_mid)
        def _():
            relay_w(u)

            @pl.when(u >= 1)
            def _():
                relay_piece(u - 1)

            own_piece(u).start()

            @pl.when((u == NU - 5) | (u == NU - 2))
            def _():
                late = (u - (NU - 5)) // 3
                pieces_in(late * 2 * per, 2 * per + late * per)
                project(late * 2 * cb, 2 * cb + late * cb)

        return z

    lax.fori_loop(0, NU, step, 0)

    @pl.when(is_end)
    def _():
        for p in range(NP):
            w_z(p, to_m).wait_send()

        def drain(u, z):
            end_piece(u, to_m).wait_send()
            return z

        lax.fori_loop(0, NU, drain, 0)
        for r in range(NR):
            y_out(r, to_m).wait_recv()

    @pl.when(is_mid)
    def _():
        relay_piece(NU - 1)
        pieces_in(3 * per, NU)
        project(3 * cb, NR)
        own_y = pltpu.make_async_copy(y1, y_hbm, loc.at[0])
        own_y.start()
        w_so1.wait_send()

        def drain(u, z):
            own_piece(u).wait_send()
            passed_piece(u).wait_send()
            return z

        lax.fori_loop(0, NU, drain, 0)
        for r in range(NR):
            y_out(r, to_e).wait_send()
        for kind in kinds:
            for p in range(NP):
                w_out(kind, p).wait_send()
        own_y.wait()


def _attend_call(q, kv_all, seg_all, w):
    R, C = q.shape
    N = w.shape[1]
    BQ = R // NB
    NU = NB * (C // (2 * HEAD_DIM))
    dma = pltpu.SemaphoreType.DMA
    hbm = pl.BlockSpec(memory_space=pltpu.HBM)
    bf16, f32 = jnp.bfloat16, jnp.float32
    stat = pltpu.VMEM((2, BQ, HEAD_DIM), f32)
    return pl.pallas_call(
        _attend_out,
        out_shape=jax.ShapeDtypeStruct((R, N), bf16),
        in_specs=[hbm] * 4,
        out_specs=hbm,
        scratch_shapes=[
            pltpu.VMEM((R, C), bf16),
            pltpu.VMEM((C // (2 * HEAD_DIM), NT * R, 4 * HEAD_DIM), bf16),
            pltpu.VMEM(seg_all.shape, jnp.int32),
            pltpu.VMEM((R, HEAD_DIM), jnp.int32),
            pltpu.VMEM((2, NT * NB // 2, BQ, 2 * BQ), f32),
            stat, stat, stat,
            pltpu.VMEM((NT, R, C), bf16),
            pltpu.VMEM((NT, C, N), bf16),
            pltpu.VMEM((NT, C, N), bf16),
            pltpu.VMEM((R, N), bf16),
            pltpu.VMEM((R, N), bf16),
            dma((5,)), dma((C // (2 * HEAD_DIM), NT)), dma((11, NP)), dma((11, NP)), dma((2, NU)), dma((2, NU)), dma((NU,)), dma((NU,)),
            dma((NP,)), dma((NP,)), dma((NR,)), dma((NR,)),
        ],
        compiler_params=pltpu.CompilerParams(collective_id=1, has_side_effects=True, vmem_limit_bytes=62 * MIB),
        cost_estimate=pl.CostEstimate(flops=4 * R * NT * C * N, bytes_accessed=2 * NT * (R * C + C * N), transcendentals=R * NT * R * 4),
        name="attend_out",
    )(q, kv_all, seg_all, w)


def solution(mesh):
    def local_block(x_blk, wqkv_blk, wout_blk, seg_blk):
        q, kv_all, seg_all = _gather_call(True, x_blk, wqkv_blk, seg_blk.reshape(-1, 128))
        return _attend_call(q, kv_all, seg_all.reshape(-1, 128), wout_blk)

    row_spec = P(("dp", "sp"), "tp")
    return jax.shard_map(local_block, mesh=mesh, in_specs=(row_spec, P("sp", "tp"), P("sp", "tp"), P(("dp", "sp"))), out_specs=row_spec, check_vma=False)
```

```python
import functools

import jax
import jax.numpy as jnp
from jax import lax
from jax.experimental import pallas as pl
from jax.experimental.pallas import tpu as pltpu
from jax.sharding import PartitionSpec as P

HEAD_DIM = 128
NT = 4
NR = 8
NB = 4
NP = 4
LOG2E = 1.4426950408889634
MIB = 1024 * 1024


def _mo(i, n):
    return pl.multiple_of(i * n, n)


def _gather_dot(qkv, x_hbm, w_hbm, seg_hbm, wo_hbm, *refs):
    if qkv:
        q_ref, kv_all, seg_all, w2_hbm = refs[:4]
        refs = refs[4:]
    else:
        (y_ref,) = refs[:1]
        refs = refs[1:]
    xg, wg = refs[:2]
    refs = refs[2:]
    if qkv:
        kv = refs[0]
        refs = refs[1:]
    loc, xs, xl, xr, ws_own, ws_y, ws_x, ws_f, wr_own, wr_y, wr_x, wr_f = refs[:12]
    if qkv:
        kv_send, kv_yr, kv_cr, kv_fs, kv_fr, seg_s, seg_r, z_s, z_r, zx_s, zx_r = refs[12:]

    R, C = x_hbm.shape
    N = w_hbm.shape[1]
    RC, NG, NH = R // NR, N // NP, N // (2 * NP)
    d, t, s = lax.axis_index("dp"), lax.axis_index("tp"), lax.axis_index("sp")
    yc, c = s // 2, s % 2
    sib, ynb, diag = s + 1 - 2 * c, s + 2 - 4 * yc, (2 - 2 * yc) + (1 - c)
    mesh_id = pl.DeviceIdType.MESH
    to_sib, to_y, to_diag = (d, t, sib), (d, t, ynb), (d, t, diag)
    to_x = (1 - d, t, s)
    to_right, to_left = (d, t + 1, s), (d, t - 1, s)
    has_right, has_left = t < NT - 1, t > 0

    bar = pltpu.get_barrier_semaphore()

    def greet(who):
        pl.semaphore_signal(bar, inc=1, device_id=who, device_id_type=mesh_id)

    greet(to_sib)
    greet(to_y)
    greet(to_x)
    if qkv:
        greet(to_diag)

    @pl.when(has_right)
    def _():
        greet(to_right)

    @pl.when(has_left)
    def _():
        greet(to_left)

    base = 4 if qkv else 3

    @pl.when(has_right & has_left)
    def _():
        pl.semaphore_wait(bar, base + 2)

    @pl.when(jnp.logical_not(has_right & has_left))
    def _():
        pl.semaphore_wait(bar, base + 1)

    def remote(src, dst, send, recv, who):
        return pltpu.make_async_remote_copy(src, dst, send, recv, device_id=who, device_id_type=mesh_id)

    def w_own(p):
        cols = pl.ds(p * NG, NG)
        return remote(w_hbm.at[:, cols], wg.at[s, :, cols], ws_own.at[p], wr_own.at[p], to_sib)

    def w_own_in(p):
        cols = pl.ds(p * NG, NG)
        return remote(w_hbm.at[:, cols], wg.at[sib, :, cols], ws_own.at[p], wr_own.at[p], to_sib)

    def mine(p):
        return pl.ds(_mo(2 * p + d, NH), NH)

    def other(p):
        return pl.ds(_mo(2 * p + 1 - d, NH), NH)

    def w_y(p):
        return remote(w_hbm.at[:, mine(p)], wg.at[s, :, mine(p)], ws_y.at[p], wr_y.at[p], to_y)

    def w_y_in(p):
        return remote(w_hbm.at[:, mine(p)], wg.at[ynb, :, mine(p)], ws_y.at[p], wr_y.at[p], to_y)

    def w_x(p):
        return remote(wg.at[ynb, :, mine(p)], wg.at[ynb, :, mine(p)], ws_x.at[p], wr_x.at[p], to_x)

    def w_x_in(p):
        return remote(wg.at[ynb, :, other(p)], wg.at[ynb, :, other(p)], ws_x.at[p], wr_x.at[p], to_x)

    def w_f(p, which):
        cols = mine(p) if which == 0 else other(p)
        return remote(wg.at[ynb, :, cols], wg.at[ynb, :, cols], ws_f.at[which, p], wr_f.at[which, p], to_sib)

    def w_f_in(p, which):
        cols = mine(p) if which == 0 else other(p)
        return remote(wg.at[diag, :, cols], wg.at[diag, :, cols], ws_f.at[which, p], wr_f.at[which, p], to_sib)

    def rows(r):
        return pl.ds(_mo(r, RC), RC)

    def x_own(r, way):
        recv = xl if way == 0 else xr
        return remote(x_hbm.at[rows(r)], xg.at[t, rows(r)], xs.at[way, 0, r], recv.at[0, r], to_right if way == 0 else to_left)

    def x_arrive(r, way, dist):
        k = t - dist if way == 0 else t + dist
        recv = xl if way == 0 else xr
        return remote(xg.at[k, rows(r)], xg.at[k, rows(r)], xs.at[way, 0, r], recv.at[dist - 1, r], to_right if way == 0 else to_left)

    def x_forward(r, way, dist):
        k = t - dist if way == 0 else t + dist
        recv = xl if way == 0 else xr
        return remote(xg.at[k, rows(r)], xg.at[k, rows(r)], xs.at[way, dist, r], recv.at[dist, r], to_right if way == 0 else to_left)

    def send_own_x(r):
        @pl.when(has_right)
        def _():
            x_own(r, 0).start()

        @pl.when(has_left)
        def _():
            x_own(r, 1).start()

    def relay_x(r):
        for dist in range(1, NT):
            for way in range(2):
                here = (t >= dist) if way == 0 else (t <= NT - 1 - dist)

                @pl.when(here)
                def _():
                    x_arrive(r, way, dist).wait_recv()
                    if dist < NT - 1:
                        @pl.when(has_right if way == 0 else has_left)
                        def _():
                            x_forward(r, way, dist).start()

    own_x = pltpu.make_async_copy(x_hbm, xg.at[t], loc.at[0])
    own_w = pltpu.make_async_copy(w_hbm, wg.at[s], loc.at[1])
    for r in range(2):
        send_own_x(r)
    for p in range(NP):
        w_y(p).start()
    for p in range(NP):
        w_own(p).start()
    own_x.start()
    own_w.start()
    if qkv:
        own_seg = pltpu.make_async_copy(seg_hbm, seg_all.at[s], loc.at[3])
        own_seg.start()
        peers = ((to_sib, sib), (to_y, ynb), (to_diag, diag))

        def seg_out(i):
            return remote(seg_hbm, seg_all.at[s], seg_s.at[i], seg_r.at[i], peers[i][0])

        def seg_in(i):
            return remote(seg_hbm, seg_all.at[peers[i][1]], seg_s.at[i], seg_r.at[i], peers[i][0])

        for i in range(3):
            seg_out(i).start()

    def unit(r, p):
        cols = pl.ds(_mo(p, NG), NG)
        acc = jnp.dot(xg[0, rows(r), :], wg[0, :, cols], preferred_element_type=jnp.float32)
        for k in range(1, NT):
            acc += jnp.dot(xg[k, rows(r), :], wg[k, :, cols], preferred_element_type=jnp.float32)
        out = acc.astype(jnp.bfloat16)
        if qkv:
            for h in range(2):
                at = 3 * HEAD_DIM * h
                q_ref[rows(r), pl.ds(pl.multiple_of(p * (2 * HEAD_DIM) + h * HEAD_DIM, HEAD_DIM), HEAD_DIM)] = out[:, at : at + HEAD_DIM]
                kv[rows(r), pl.ds(_mo(2 * p + h, 2 * HEAD_DIM), 2 * HEAD_DIM)] = out[:, at + HEAD_DIM : at + 3 * HEAD_DIM]
        else:
            y_ref[rows(r), cols] = out

    def kv_cols(p):
        return pl.ds(_mo(p, 4 * HEAD_DIM), 4 * HEAD_DIM)

    def kv_unit(r, p, who, send, recv):
        return remote(kv.at[rows(r), kv_cols(p)], kv_all.at[s, rows(r), kv_cols(p)], send, recv, who)

    def send_unit(r, p):
        pltpu.make_async_copy(kv.at[rows(r), kv_cols(p)], kv_all.at[s, rows(r), kv_cols(p)], loc.at[2]).start()

        @pl.when(yc == 0)
        def _():
            kv_unit(r, p, to_y, kv_send.at[0], kv_yr.at[r]).start()

        @pl.when(c == 0)
        def _():
            kv_unit(r, p, to_sib, kv_send.at[1], kv_cr.at[r]).start()

    def do_units(work):
        for n, f in work:
            def body(u, z, f=f):
                unit(*f(u))
                return z
            lax.fori_loop(0, n, body, 0)
        if qkv:
            for n, f in work:
                def body(u, z, f=f):
                    send_unit(*f(u))
                    return z
                lax.fori_loop(0, n, body, 0)

    def kv_row(r, owner, who, send, recv):
        return remote(kv_all.at[owner, rows(r)], kv_all.at[owner, rows(r)], send, recv, who)

    def pass_kv(r):
        if qkv:
            @pl.when(yc == 1)
            def _():
                kv_row(r, ynb, to_y, kv_fs.at[r], kv_yr.at[r]).wait_recv()
                kv_row(r, ynb, to_sib, kv_fs.at[r], kv_fr.at[r]).start()

    is_end = (t == 0) | (t == NT - 1)
    is_mid = jnp.logical_not(is_end)
    N2 = wo_hbm.shape[1] // (2 * NP)

    def half_cols(p, mine_cols):
        return pl.ds(_mo(2 * p + d, N2) if mine_cols else _mo(2 * p + 1 - d, N2), N2)

    def z_out(p):
        at = half_cols(p, True)
        return remote(wo_hbm.at[:, at], w2_hbm.at[:, at], z_s.at[p], z_r.at[p], (d, (t + 3) // 3, s))

    def z_in(p):
        at = half_cols(p, True)
        return remote(w2_hbm.at[:, at], w2_hbm.at[:, at], z_s.at[p], z_r.at[p], to_x)

    def zx(p, mine_cols):
        at = half_cols(p, mine_cols)
        return remote(w2_hbm.at[:, at], w2_hbm.at[:, at], zx_s.at[p], zx_r.at[p], to_x)

    def relay_w(i):
        if qkv and i < NP:
            @pl.when(is_end)
            def _():
                z_out(i).start()
        if i < NP:
            w_y_in(i).wait_recv()
            w_x(i).start()
            w_f(i, 0).start()
        if 1 <= i <= NP:
            w_x_in(i - 1).wait_recv()
            w_f(i - 1, 1).start()
            p = i - 1
            if p == 0:
                own_x.wait()
                own_w.wait()
            w_own_in(p).wait_recv()
            w_f_in(p, 0).wait_recv()
            w_f_in(p, 1).wait_recv()

    for i in range(NP + 1):
        relay_x(i)
        send_own_x(i + 2)
        relay_w(i)
        if i == 2:
            do_units([(6, lambda u: (u // 2, u % 2))])
        if i == 3:
            do_units([(2, lambda u: (3, u)), (4, lambda u: (u, 2))])
        if i == 4:
            do_units([(3, lambda u: (4, u)), (5, lambda u: (u, 3))])

    def late(i, z):
        relay_x(i)

        @pl.when(i + 2 < NR)
        def _():
            send_own_x(i + 2)

        pass_kv(2 * (i - NP - 1))
        pass_kv(2 * (i - NP - 1) + 1)

        @pl.when(is_mid & (i < NP + 3))
        def _():
            for p in range(2):
                z_in(2 * (i - NP - 1) + p).wait_recv()
                zx(2 * (i - NP - 1) + p, True).start()

        do_units([(NP, lambda u: (i, u))])
        return z

    lax.fori_loop(NP + 1, NR, late, 0)

    for p in range(NP):
        w_own(p).wait_send()
        w_y(p).wait_send()
        w_x(p).wait_send()
        w_f(p, 0).wait_send()
        w_f(p, 1).wait_send()

    def drain_x(r, z):
        @pl.when(has_right)
        def _():
            x_own(r, 0).wait_send()
            for dist in range(1, NT - 1):
                @pl.when(t >= dist)
                def _():
                    x_forward(r, 0, dist).wait_send()

        @pl.when(has_left)
        def _():
            x_own(r, 1).wait_send()
            for dist in range(1, NT - 1):
                @pl.when(t <= NT - 1 - dist)
                def _():
                    x_forward(r, 1, dist).wait_send()

        return z

    lax.fori_loop(0, NR, drain_x, 0)
    if qkv:
        pass_kv(6)
        pass_kv(7)

        @pl.when(is_end)
        def _():
            for p in range(NP):
                z_out(p).wait_send()

        @pl.when(is_mid)
        def _():
            for p in range(NP):
                zx(p, True).wait_send()
                zx(p, False).wait_recv()

        own_seg.wait()
        for i in range(3):
            seg_out(i).wait_send()
            seg_in(i).wait_recv()
        pltpu.make_async_copy(kv, kv_all.at[s], loc.at[2]).wait()

        @pl.when(yc == 0)
        def _():
            remote(kv, kv_all.at[s], kv_send.at[0], kv_yr.at[0], to_y).wait_send()

        @pl.when(c == 0)
        def _():
            remote(kv, kv_all.at[s], kv_send.at[1], kv_cr.at[0], to_sib).wait_send()

        def drain_kv(r, z):
            @pl.when(c == 1)
            def _():
                kv_row(r, sib, to_sib, kv_fs.at[r], kv_cr.at[r]).wait_recv()

            @pl.when(yc == 1)
            def _():
                kv_row(r, ynb, to_sib, kv_fs.at[r], kv_fr.at[r]).wait_send()
                kv_row(r, diag, to_sib, kv_fs.at[r], kv_fr.at[r]).wait_recv()

            return z

        lax.fori_loop(0, NR, drain_kv, 0)


def _gather_call(qkv, x, w, seg, wo):
    R, C = x.shape
    N = w.shape[1]
    dma = pltpu.SemaphoreType.DMA
    hbm = pl.BlockSpec(memory_space=pltpu.HBM)
    vmem = pl.BlockSpec(memory_space=pltpu.VMEM)
    bf16 = jnp.bfloat16
    scratch = [pltpu.VMEM((NT, R, C), bf16), pltpu.VMEM((NT, C, N), bf16)]
    if qkv:
        heads = N // (3 * HEAD_DIM)
        out_shape = (
            jax.ShapeDtypeStruct((R, heads * HEAD_DIM), bf16),
            jax.ShapeDtypeStruct((NT, R, 2 * heads * HEAD_DIM), bf16),
            jax.ShapeDtypeStruct((NT,) + seg.shape, jnp.int32),
            jax.ShapeDtypeStruct(wo.shape, bf16),
        )
        out_specs = (vmem, hbm, hbm, hbm)
        scratch.append(pltpu.VMEM((R, 2 * heads * HEAD_DIM), bf16))
    else:
        out_shape = jax.ShapeDtypeStruct((R, N), bf16)
        out_specs = vmem
    scratch += [dma((4,)), dma((2, 3, NR)), dma((3, NR)), dma((3, NR)), dma((NP,)), dma((NP,)), dma((NP,)), dma((2, NP)),
                dma((NP,)), dma((NP,)), dma((NP,)), dma((2, NP))]
    if qkv:
        scratch += [dma((2,)), dma((NR,)), dma((NR,)), dma((NR,)), dma((NR,)), dma((3,)), dma((3,)), dma((NP,)), dma((NP,)), dma((NP,)), dma((NP,))]
    return pl.pallas_call(
        functools.partial(_gather_dot, qkv),
        out_shape=out_shape,
        in_specs=[hbm] * 4,
        out_specs=out_specs,
        scratch_shapes=scratch,
        compiler_params=pltpu.CompilerParams(collective_id=0 if qkv else 1, has_side_effects=True, vmem_limit_bytes=60 * MIB),
        cost_estimate=pl.CostEstimate(flops=2 * R * NT * C * N, bytes_accessed=2 * NT * (R * C + C * N), transcendentals=0),
        name="qkv_dot" if qkv else "out_dot",
    )(x, w, seg, wo)


def _attend_out(q_hbm, kv_hbm, seg_hbm, w_hbm, w2_hbm, y_hbm, q_ref, kv_ref, seg_ref, first_ref, sc0, sc1, m0, m1, l0, l1, acc_ref, xg, wg, wg2,
                y1, y2, loc, kv_sem, w_send, w_recv, o_send, o_recv, e_send, e_recv, y_send, y_recv):
    R, C = q_hbm.shape
    N = w_hbm.shape[1]
    RC, NH = R // NR, N // (2 * NP)
    BQ = R // NB
    BK = 2 * BQ
    H = C // HEAD_DIM
    CP = 2 * HEAD_DIM
    per = C // CP
    NU = NB * per
    d, t, s = lax.axis_index("dp"), lax.axis_index("tp"), lax.axis_index("sp")
    yc, c = s // 2, s % 2
    sib, ynb, diag = s + 1 - 2 * c, s + 2 - 4 * yc, (2 - 2 * yc) + (1 - c)
    mesh_id = pl.DeviceIdType.MESH
    to_sib, to_y, to_x = (d, t, sib), (d, t, ynb), (1 - d, t, s)
    is_end = (t == 0) | (t == NT - 1)
    is_mid = jnp.logical_not(is_end)
    e, o = 3 * t - 3, 3 - t
    oe = 3 - e
    to_m, to_e, to_o = (d, (t + 3) // 3, s), (d, e, s), (d, o, s)
    bar = pltpu.get_barrier_semaphore()

    def greet(who):
        pl.semaphore_signal(bar, inc=1, device_id=who, device_id_type=mesh_id)

    def remote(src, dst, send, recv, who):
        return pltpu.make_async_remote_copy(src, dst, send, recv, device_id=who, device_id_type=mesh_id)

    def rows(r):
        return pl.ds(_mo(r, RC), RC)

    def mine(p):
        return pl.ds(_mo(2 * p + d, NH), NH)

    def other(p):
        return pl.ds(_mo(2 * p + 1 - d, NH), NH)

    def piece(k, u):
        return xg.at[k, pl.ds(_mo(u // per, BQ), BQ), pl.ds(_mo(u % per, CP), CP)]

    kinds = {
        "y": (s, mine, to_y, ynb, mine),
        "x": (ynb, mine, to_x, ynb, other),
        "sy": (ynb, mine, to_sib, diag, mine),
        "sx": (ynb, other, to_sib, diag, other),
    }
    number = {kind: i for i, kind in enumerate(kinds)}
    panels = ((w_hbm, wg), (w2_hbm, wg2))

    def w_out(i, kind, p):
        hbm, panel = panels[i]
        owner, cols, who, _, _ = kinds[kind]
        n = number[kind]
        src = hbm.at[:, cols(p)] if kind == "y" else panel.at[owner, :, cols(p)]
        return remote(src, panel.at[owner, :, cols(p)], w_send.at[i, n, p], w_recv.at[i, n, p], who)

    def w_in(i, kind, p):
        _, _, who, owner, cols = kinds[kind]
        n = number[kind]
        at = panels[i][1].at[owner, :, cols(p)]
        return remote(at, at, w_send.at[i, n, p], w_recv.at[i, n, p], who)

    def w_sib(i, owner):
        return remote(panels[i][0], panels[i][1].at[owner], loc.at[4 + i], loc.at[6 + i], to_sib)

    def w_own(i):
        return pltpu.make_async_copy(panels[i][0], panels[i][1].at[s], loc.at[2 + i])

    def end_piece(u, who):
        k = t if who is to_m else e
        return remote(piece(k, u), piece(k, u), e_send.at[u], e_recv.at[u], who)

    def own_piece(u):
        return remote(piece(t, u), piece(t, u), o_send.at[0, u], o_recv.at[0, u], to_o)

    def passed_piece(u):
        return remote(piece(e, u), piece(e, u), o_send.at[1, u], o_recv.at[1, u], to_o)

    def piece_in(i, u):
        k = o if i == 0 else oe
        return remote(piece(k, u), piece(k, u), o_send.at[i, u], o_recv.at[i, u], to_o)

    def y_out(r, who):
        return remote(y2.at[rows(r)], y_hbm.at[rows(r)], y_send.at[r], y_recv.at[r], who)

    q_copy = pltpu.make_async_copy(q_hbm, q_ref, loc.at[0])
    seg_copy = pltpu.make_async_copy(seg_hbm, seg_ref, loc.at[1])

    def kv_copy(h, k):
        return pltpu.make_async_copy(kv_hbm.at[k, :, pl.ds(_mo(h, CP), CP)], kv_ref.at[h, pl.ds(_mo(k, R), R)], kv_sem.at[h, k])

    seg_copy.start()
    q_copy.start()
    for h in range(H):
        for k in range(NT):
            @pl.when(k <= s)
            def _():
                kv_copy(h, k).start()

    @pl.when(is_end)
    def _():
        greet(to_m)
        pl.semaphore_wait(bar, 1)

    @pl.when(is_mid)
    def _():
        for who in (to_e, to_o, to_y, to_x, to_sib):
            greet(who)
        pl.semaphore_wait(bar, 5)
        for i in (1, 0):
            for p in range(NP):
                w_out(i, "y", p).start()
        for i in (1, 0):
            w_sib(i, s).start()
            w_own(i).start()

    seg_copy.wait()
    seg = seg_ref[...]
    starts = [jnp.sum(jnp.where(seg < doc, 1.0, 0.0), axis=(0, 1), keepdims=True) for doc in range(1, 4)]

    def first_rows(b, z):
        row = (s * R + b * BQ + lax.broadcasted_iota(jnp.int32, (BQ, HEAD_DIM), 0)).astype(jnp.float32)
        out = jnp.zeros((BQ, HEAD_DIM), jnp.float32)
        for start in starts:
            out = jnp.where(start <= row, jnp.maximum(out, start), out)
        first_ref[pl.ds(_mo(b, BQ), BQ), :] = out.astype(jnp.int32)
        return z

    lax.fori_loop(0, NB, first_rows, 0)
    q_copy.wait()

    scale = LOG2E / HEAD_DIM ** 0.5
    sc, m_refs, l_refs = (sc0, sc1), (m0, m1), (l0, l1)

    def lane_groups(a, op):
        out = a[:, :HEAD_DIM]
        for g in range(1, a.shape[1] // HEAD_DIM):
            out = op(out, a[:, HEAD_DIM * g : HEAD_DIM * (g + 1)])
        return out

    def wide(a):
        return jnp.concatenate([a] * (BK // HEAD_DIM), axis=1)

    def attend(half, k, par, stages):
        full = 2 * s + half
        b, h = 2 * half + k // H, k % H
        q_at = pl.ds(_mo(b, BQ), BQ)
        b3, h3 = 2 * half + (k - 2) // H, (k - 2) % H
        if 1 in stages:
            m_refs[par][...] = jnp.full((BQ, HEAD_DIM), -3e38, jnp.float32)
        if 2 in stages:
            l_refs[1 - par][...] = jnp.zeros((BQ, HEAD_DIM), jnp.float32)
        if 3 in stages:
            acc_ref[...] = jnp.zeros((BQ, HEAD_DIM), jnp.float32)

        def tile(j, z, width, diagonal):
            if 3 in stages:
                acc = acc_ref[...]
                scale_l = wide(l_refs[par][...])
                for i in range(width):
                    p = (sc[par][j + i] * scale_l).astype(jnp.bfloat16)
                    acc += jnp.dot(p, kv_ref[h3, pl.ds(_mo(j + i, BK), BK), HEAD_DIM:], preferred_element_type=jnp.float32)
                acc_ref[...] = acc
            if 1 in stages:
                q = q_ref[q_at, pl.ds(_mo(h, HEAD_DIM), HEAD_DIM)]
                first = wide(first_ref[q_at, :])
                m = m_refs[par][...]
                for i in range(width):
                    a = lax.dot_general(q, kv_ref[h, pl.ds(_mo(j + i, BK), BK), :HEAD_DIM], (((1,), (1,)), ((), ())), preferred_element_type=jnp.float32)
                    key_id = (j + i) * BK + lax.broadcasted_iota(jnp.int32, (BQ, BK), 1)
                    seen = key_id >= first
                    if diagonal:
                        seen = seen & (key_id <= s * R + b * BQ + lax.broadcasted_iota(jnp.int32, (BQ, BK), 0))
                    a = jnp.where(seen, a, -jnp.inf)
                    sc[par][j + i] = a
                    m = jnp.maximum(m, lane_groups(a, jnp.maximum))
                m_refs[par][...] = m
            if 2 in stages:
                top = wide(m_refs[1 - par][...])
                l = l_refs[1 - par][...]
                for i in range(width):
                    w = jnp.exp2((sc[1 - par][j + i] - top) * scale)
                    sc[1 - par][j + i] = w
                    l += lane_groups(w, jnp.add)
                l_refs[1 - par][...] = l
            return z

        lax.fori_loop(0, s, lambda i, z: tile(2 * i, z, 2, False), 0)
        lax.fori_loop(0, half, lambda i, z: tile(2 * s, z, 1, False), 0)
        tile(full, 0, 1, True)
        if 1 in stages:
            m_refs[par][...] = jnp.broadcast_to(jnp.max(m_refs[par][...], axis=1, keepdims=True), (BQ, HEAD_DIM))
        if 2 in stages:
            l_refs[1 - par][...] = jnp.broadcast_to(1.0 / jnp.sum(l_refs[1 - par][...], axis=1, keepdims=True), (BQ, HEAD_DIM))
        if 3 in stages:
            xg[t, pl.ds(_mo(b3, BQ), BQ), pl.ds(_mo(h3, HEAD_DIM), HEAD_DIM)] = acc_ref[...].astype(jnp.bfloat16)

    def dot_rows(panel, out, r):
        acc = jnp.dot(xg[0, rows(r), :], panel[0], preferred_element_type=jnp.float32)
        for k in range(1, NT):
            acc += jnp.dot(xg[k, rows(r), :], panel[k], preferred_element_type=jnp.float32)
        out[rows(r), :] = acc.astype(jnp.bfloat16)

    def relay_piece(u):
        end_piece(u, to_e).wait_recv()
        passed_piece(u).start()

    def relay_w(i, kind, p):
        w_in(i, kind, p).wait_recv()
        if kind == "y":
            w_out(i, "x", p).start()
            w_out(i, "sy", p).start()
        else:
            w_out(i, "sx", p).start()

    plan = ((1, "y", 6), (1, "x", 11), (0, "y", 21), (0, "x", 26))
    steps = H * 2 + 2

    def after(half, k):
        g = half * steps + k
        for i, kind, base in plan:
            @pl.when(is_mid & (g >= base) & (g < base + 4 * NP) & ((g - base) % 4 == 0))
            def _():
                relay_w(i, kind, (g - base) // 4)

    def finished(u):
        @pl.when(is_end)
        def _():
            end_piece(u, to_m).start()

        @pl.when(is_mid)
        def _():
            @pl.when(u >= 1)
            def _():
                relay_piece(u - 1)

            own_piece(u).start()

    def kv_here(half, k):
        @pl.when((half == 0) & (k < H))
        def _():
            for owner in range(NT):
                @pl.when(owner <= s)
                def _():
                    kv_copy(k, owner).wait()

    def panel_here(i):
        w_own(i).wait()
        w_sib(i, sib).wait_recv()
        for kind in ("sy", "sx"):
            for p in range(NP):
                w_in(i, kind, p).wait_recv()

    def end_columns(b, n):
        for u in range(n * per):
            piece_in(0, b * per + u).wait_recv()
            piece_in(1, b * per + u).wait_recv()
        lo, hi = b * (BQ // RC), (b + n) * (BQ // RC)

        def chunk(r, z):
            dot_rows(wg2, y2, r)

            @pl.when(r > lo)
            def _():
                y_out(r - 1, to_e).start()

            return z

        lax.fori_loop(lo, hi, chunk, 0)

    def half_rows(half, z):
        kv_here(half, 0)
        attend(half, 0, 0, (1,))
        after(half, 0)
        kv_here(half, 1)
        attend(half, 1, 1, (1, 2))
        after(half, 1)

        def pair(i, z):
            for par in range(2):
                k = 2 * i + par
                kv_here(half, k)
                attend(half, k, par, (1, 2, 3))
                after(half, k)
            finished(half * 2 * per + i - 1)

            @pl.when(is_mid & (half == 1) & (i == 4))
            def _():
                panel_here(1)
                end_columns(0, 2)

            @pl.when(is_mid & (half == 1) & (i == 5))
            def _():
                y_out(2 * (BQ // RC) - 1, to_e).start()

            @pl.when(is_mid & (half == 1) & (i == H - 1))
            def _():
                end_columns(2, 1)

            return z

        lax.fori_loop(1, H, pair, 0)
        attend(half, 2 * H, 0, (2, 3))
        after(half, 2 * H)
        attend(half, 2 * H + 1, 1, (3,))
        after(half, 2 * H + 1)
        finished(half * 2 * per + 2 * per - 1)
        return z

    lax.fori_loop(0, NB // 2, half_rows, 0)

    @pl.when(is_end)
    def _():
        def drain(u, z):
            end_piece(u, to_m).wait_send()
            return z

        lax.fori_loop(0, NU, drain, 0)
        for r in range(NR):
            y_out(r, to_m).wait_recv()

    @pl.when(is_mid)
    def _():
        relay_piece(NU - 1)
        for i, kind, base in plan:
            for p in range(NP):
                if base + 4 * p >= 2 * steps:
                    relay_w(i, kind, p)

        y_out(3 * (BQ // RC) - 1, to_e).start()
        panel_here(0)
        end_columns(3, 1)

        def own_columns(r, z):
            dot_rows(wg, y1, r)

            @pl.when(r == 0)
            def _():
                y_out(NR - 1, to_e).start()

            return z

        lax.fori_loop(0, NR, own_columns, 0)
        own_y = pltpu.make_async_copy(y1, y_hbm, loc.at[0])
        own_y.start()

        def drain(u, z):
            own_piece(u).wait_send()
            passed_piece(u).wait_send()
            return z

        lax.fori_loop(0, NU, drain, 0)
        for r in range(NR):
            y_out(r, to_e).wait_send()
        for i in range(2):
            w_sib(i, s).wait_send()
            for kind in kinds:
                for p in range(NP):
                    w_out(i, kind, p).wait_send()
        own_y.wait()


def _attend_call(q, kv_all, seg_all, w, w2):
    R, C = q.shape
    N = w.shape[1]
    BQ = R // NB
    NU = NB * (C // (2 * HEAD_DIM))
    dma = pltpu.SemaphoreType.DMA
    hbm = pl.BlockSpec(memory_space=pltpu.HBM)
    bf16, f32 = jnp.bfloat16, jnp.float32
    stat = pltpu.VMEM((BQ, HEAD_DIM), f32)
    scores = pltpu.VMEM((NT * NB // 2, BQ, 2 * BQ), f32)
    return pl.pallas_call(
        _attend_out,
        out_shape=jax.ShapeDtypeStruct((R, N), bf16),
        in_specs=[hbm] * 5,
        out_specs=hbm,
        scratch_shapes=[
            pltpu.VMEM((R, C), bf16),
            pltpu.VMEM((C // HEAD_DIM, NT * R, 2 * HEAD_DIM), bf16),
            pltpu.VMEM(seg_all.shape, jnp.int32),
            pltpu.VMEM((R, HEAD_DIM), jnp.int32),
            scores, scores, stat, stat, stat, stat, stat,
            pltpu.VMEM((NT, R, C), bf16),
            pltpu.VMEM((NT, C, N), bf16),
            pltpu.VMEM((NT, C, N), bf16),
            pltpu.VMEM((R, N), bf16),
            pltpu.VMEM((R, N), bf16),
            dma((8,)), dma((C // HEAD_DIM, NT)), dma((2, 4, NP)), dma((2, 4, NP)), dma((2, NU)), dma((2, NU)), dma((NU,)), dma((NU,)),
            dma((NR,)), dma((NR,)),
        ],
        compiler_params=pltpu.CompilerParams(collective_id=1, has_side_effects=True, vmem_limit_bytes=62 * MIB),
        cost_estimate=pl.CostEstimate(flops=4 * R * NT * C * N, bytes_accessed=2 * NT * (R * C + C * N), transcendentals=R * NT * R * 4),
        name="attend_out",
    )(q, kv_all, seg_all, w, w2)


def solution(mesh):
    def local_block(x_blk, wqkv_blk, wout_blk, seg_blk):
        q, kv_all, seg_all, w2 = _gather_call(True, x_blk, wqkv_blk, seg_blk.reshape(-1, 128), wout_blk)
        return _attend_call(q, kv_all, seg_all.reshape(-1, 128), wout_blk, w2)

    row_spec = P(("dp", "sp"), "tp")
    return jax.shard_map(local_block, mesh=mesh, in_specs=(row_spec, P("sp", "tp"), P("sp", "tp"), P(("dp", "sp"))), out_specs=row_spec, check_vma=False)
```

```python
import functools

import jax
import jax.numpy as jnp
from jax import lax
from jax.experimental import pallas as pl
from jax.experimental.pallas import tpu as pltpu
from jax.sharding import PartitionSpec as P

HEAD_DIM = 128
NT = 4
NR = 8
NB = 4
AHEAD = 2
LATE = 1
NP = 4
LOG2E = 1.4426950408889634
MIB = 1024 * 1024


def _mo(i, n):
    return pl.multiple_of(i * n, n)


def _gather_dot(qkv, x_hbm, w_hbm, seg_hbm, wo_hbm, *refs):
    if qkv:
        q_ref, kv_all, seg_all, w2_hbm = refs[:4]
        refs = refs[4:]
    else:
        (y_ref,) = refs[:1]
        refs = refs[1:]
    xg, wg = refs[:2]
    refs = refs[2:]
    if qkv:
        kv = refs[0]
        refs = refs[1:]
    loc, xs, xl, xr, ws_own, ws_y, ws_x, ws_f, wr_own, wr_y, wr_x, wr_f = refs[:12]
    if qkv:
        kv_send, kv_yr, kv_cr, kv_fs, kv_fr, seg_s, seg_r, z_s, z_r, zx_s, zx_r = refs[12:]

    R, C = x_hbm.shape
    N = w_hbm.shape[1]
    RC, NG, NH = R // NR, N // NP, N // (2 * NP)
    d, t, s = lax.axis_index("dp"), lax.axis_index("tp"), lax.axis_index("sp")
    yc, c = s // 2, s % 2
    sib, ynb, diag = s + 1 - 2 * c, s + 2 - 4 * yc, (2 - 2 * yc) + (1 - c)
    mesh_id = pl.DeviceIdType.MESH
    to_sib, to_y, to_diag = (d, t, sib), (d, t, ynb), (d, t, diag)
    to_x = (1 - d, t, s)
    to_right, to_left = (d, t + 1, s), (d, t - 1, s)
    has_right, has_left = t < NT - 1, t > 0

    bar = pltpu.get_barrier_semaphore()

    def greet(who):
        pl.semaphore_signal(bar, inc=1, device_id=who, device_id_type=mesh_id)

    greet(to_sib)
    greet(to_y)
    greet(to_x)
    if qkv:
        greet(to_diag)

    @pl.when(has_right)
    def _():
        greet(to_right)

    @pl.when(has_left)
    def _():
        greet(to_left)

    base = 4 if qkv else 3

    @pl.when(has_right & has_left)
    def _():
        pl.semaphore_wait(bar, base + 2)

    @pl.when(jnp.logical_not(has_right & has_left))
    def _():
        pl.semaphore_wait(bar, base + 1)

    def remote(src, dst, send, recv, who):
        return pltpu.make_async_remote_copy(src, dst, send, recv, device_id=who, device_id_type=mesh_id)

    def w_own(p):
        cols = pl.ds(p * NG, NG)
        return remote(w_hbm.at[:, cols], wg.at[s, :, cols], ws_own.at[p], wr_own.at[p], to_sib)

    def w_own_in(p):
        cols = pl.ds(p * NG, NG)
        return remote(w_hbm.at[:, cols], wg.at[sib, :, cols], ws_own.at[p], wr_own.at[p], to_sib)

    def mine(p):
        return pl.ds(_mo(2 * p + d, NH), NH)

    def other(p):
        return pl.ds(_mo(2 * p + 1 - d, NH), NH)

    def w_y(p):
        return remote(w_hbm.at[:, mine(p)], wg.at[s, :, mine(p)], ws_y.at[p], wr_y.at[p], to_y)

    def w_y_in(p):
        return remote(w_hbm.at[:, mine(p)], wg.at[ynb, :, mine(p)], ws_y.at[p], wr_y.at[p], to_y)

    def w_x(p):
        return remote(wg.at[ynb, :, mine(p)], wg.at[ynb, :, mine(p)], ws_x.at[p], wr_x.at[p], to_x)

    def w_x_in(p):
        return remote(wg.at[ynb, :, other(p)], wg.at[ynb, :, other(p)], ws_x.at[p], wr_x.at[p], to_x)

    def w_f(p, which):
        cols = mine(p) if which == 0 else other(p)
        return remote(wg.at[ynb, :, cols], wg.at[ynb, :, cols], ws_f.at[which, p], wr_f.at[which, p], to_sib)

    def w_f_in(p, which):
        cols = mine(p) if which == 0 else other(p)
        return remote(wg.at[diag, :, cols], wg.at[diag, :, cols], ws_f.at[which, p], wr_f.at[which, p], to_sib)

    def rows(r):
        return pl.ds(_mo(r, RC), RC)

    def x_own(r, way):
        recv = xl if way == 0 else xr
        return remote(x_hbm.at[rows(r)], xg.at[t, rows(r)], xs.at[way, 0, r], recv.at[0, r], to_right if way == 0 else to_left)

    def x_arrive(r, way, dist):
        k = t - dist if way == 0 else t + dist
        recv = xl if way == 0 else xr
        return remote(xg.at[k, rows(r)], xg.at[k, rows(r)], xs.at[way, 0, r], recv.at[dist - 1, r], to_right if way == 0 else to_left)

    def x_forward(r, way, dist):
        k = t - dist if way == 0 else t + dist
        recv = xl if way == 0 else xr
        return remote(xg.at[k, rows(r)], xg.at[k, rows(r)], xs.at[way, dist, r], recv.at[dist, r], to_right if way == 0 else to_left)

    def send_own_x(r):
        @pl.when(has_right)
        def _():
            x_own(r, 0).start()

        @pl.when(has_left)
        def _():
            x_own(r, 1).start()

    def relay_x(i):
        for dist in range(1, NT):
            r = i - (dist - 1)
            for way in range(2):
                here = (t >= dist) if way == 0 else (t <= NT - 1 - dist)

                @pl.when(here & (r >= 0) & (r < NR))
                def _():
                    x_arrive(r, way, dist).wait_recv()
                    if dist < NT - 1:
                        @pl.when(has_right if way == 0 else has_left)
                        def _():
                            x_forward(r, way, dist).start()

            if dist == 1:
                @pl.when(jnp.int32(i + AHEAD) < NR)
                def _():
                    send_own_x(i + AHEAD)

    own_x = pltpu.make_async_copy(x_hbm, xg.at[t], loc.at[0])
    own_w = pltpu.make_async_copy(w_hbm, wg.at[s], loc.at[1])
    for r in range(AHEAD):
        send_own_x(r)
    for p in range(NP):
        w_y(p).start()
    for p in range(NP):
        w_own(p).start()
    own_x.start()
    own_w.start()
    if qkv:
        own_seg = pltpu.make_async_copy(seg_hbm, seg_all.at[s], loc.at[3])
        own_seg.start()
        peers = ((to_sib, sib), (to_y, ynb), (to_diag, diag))

        def seg_out(i):
            return remote(seg_hbm, seg_all.at[s], seg_s.at[i], seg_r.at[i], peers[i][0])

        def seg_in(i):
            return remote(seg_hbm, seg_all.at[peers[i][1]], seg_s.at[i], seg_r.at[i], peers[i][0])

        for i in range(3):
            seg_out(i).start()

    def unit(r, p):
        cols = pl.ds(_mo(p, NG), NG)
        acc = jnp.dot(xg[0, rows(r), :], wg[0, :, cols], preferred_element_type=jnp.float32)
        for k in range(1, NT):
            acc += jnp.dot(xg[k, rows(r), :], wg[k, :, cols], preferred_element_type=jnp.float32)
        out = acc.astype(jnp.bfloat16)
        if qkv:
            for h in range(2):
                at = 3 * HEAD_DIM * h
                q_ref[rows(r), pl.ds(pl.multiple_of(p * (2 * HEAD_DIM) + h * HEAD_DIM, HEAD_DIM), HEAD_DIM)] = out[:, at : at + HEAD_DIM]
                kv[rows(r), pl.ds(_mo(2 * p + h, 2 * HEAD_DIM), 2 * HEAD_DIM)] = out[:, at + HEAD_DIM : at + 3 * HEAD_DIM]
        else:
            y_ref[rows(r), cols] = out

    if qkv:
        early = kv.shape[1] - LATE * 2 * HEAD_DIM

    def kv_cols(p):
        return pl.ds(_mo(p, 4 * HEAD_DIM), 4 * HEAD_DIM)

    def kv_unit(r, p, who, send, recv):
        return remote(kv.at[rows(r), kv_cols(p)], kv_all.at[s, rows(r), kv_cols(p)], send, recv, who)

    def send_unit(r, p):
        pltpu.make_async_copy(kv.at[rows(r), kv_cols(p)], kv_all.at[s, rows(r), kv_cols(p)], loc.at[2]).start()

        @pl.when((yc == 0) & (p < NP - 1))
        def _():
            kv_unit(r, p, to_y, kv_send.at[0], kv_yr.at[r]).start()

        if LATE == 1:
            @pl.when((yc == 0) & (p == NP - 1))
            def _():
                at = pl.ds((NP - 1) * 4 * HEAD_DIM, 2 * HEAD_DIM)
                remote(kv.at[rows(r), at], kv_all.at[s, rows(r), at], kv_send.at[0], kv_yr.at[r], to_y).start()

        @pl.when(c == 0)
        def _():
            kv_unit(r, p, to_sib, kv_send.at[1], kv_cr.at[r]).start()

    def do_units(work):
        for n, f in work:
            def body(u, z, f=f):
                unit(*f(u))
                if qkv:
                    @pl.when(u > 0)
                    def _():
                        send_unit(*f(u - 1))
                return z
            lax.fori_loop(0, n, body, 0)
            if qkv:
                send_unit(*f(jnp.int32(n - 1)))

    def kv_row(r, owner, who, send, recv):
        at = pl.ds(0, early if who is not None else kv.shape[1])
        who = to_sib if who is None else who
        return remote(kv_all.at[owner, rows(r), at], kv_all.at[owner, rows(r), at], send, recv, who)

    def pass_kv(r):
        if qkv:
            @pl.when(yc == 1)
            def _():
                kv_row(r, ynb, to_y, kv_fs.at[r], kv_yr.at[r]).wait_recv()
                kv_row(r, ynb, to_sib, kv_fs.at[r], kv_fr.at[r]).start()

    is_end = (t == 0) | (t == NT - 1)
    is_mid = jnp.logical_not(is_end)
    N2 = wo_hbm.shape[1] // (2 * NP)

    def half_cols(p, mine_cols):
        return pl.ds(_mo(2 * p + d, N2) if mine_cols else _mo(2 * p + 1 - d, N2), N2)

    def z_out(p):
        at = half_cols(p, True)
        return remote(wo_hbm.at[:, at], w2_hbm.at[:, at], z_s.at[p], z_r.at[p], (d, (t + 3) // 3, s))

    def z_in(p):
        at = half_cols(p, True)
        return remote(w2_hbm.at[:, at], w2_hbm.at[:, at], z_s.at[p], z_r.at[p], to_x)

    def zx(p, mine_cols):
        at = half_cols(p, mine_cols)
        return remote(w2_hbm.at[:, at], w2_hbm.at[:, at], zx_s.at[p], zx_r.at[p], to_x)

    def relay_w(i):
        if qkv and i < NP:
            @pl.when(is_end)
            def _():
                z_out(i).start()
        if i < NP:
            w_y_in(i).wait_recv()
            w_x(i).start()
            w_f(i, 0).start()
        if 1 <= i <= NP:
            w_x_in(i - 1).wait_recv()
            w_f(i - 1, 1).start()
            p = i - 1
            if p == 0:
                own_x.wait()
                own_w.wait()
            w_own_in(p).wait_recv()
            w_f_in(p, 0).wait_recv()
            w_f_in(p, 1).wait_recv()

    LAG = NT - 2
    relay_x(jnp.int32(0))
    for i in range(NP + 1):
        relay_x(jnp.int32(i + 1))
        relay_w(i)
        if i == 2:
            do_units([(4, lambda u: (u // 2, u % 2))])
        if i == 3:
            do_units([(2, lambda u: (u, 2)), (3, lambda u: (2, u))])
        if i == 4:
            do_units([(3, lambda u: (u, 3)), (4, lambda u: (3, u))])

    def late(i, z):
        relay_x(i)
        @pl.when(i >= NP + 3)
        def _():
            pass_kv(2 * (i - NP - 3))
            pass_kv(2 * (i - NP - 3) + 1)

        @pl.when(is_mid & (i < NP + 4))
        def _():
            for p in range(2):
                z_in(2 * (i - NP - 2) + p).wait_recv()
                zx(2 * (i - NP - 2) + p, True).start()

        do_units([(NP, lambda u: (i - LAG, u))])
        return z

    lax.fori_loop(NP + 2, NR + LAG, late, 0)

    for p in range(NP):
        w_own(p).wait_send()
        w_y(p).wait_send()
        w_x(p).wait_send()
        w_f(p, 0).wait_send()
        w_f(p, 1).wait_send()

    def drain_x(r, z):
        @pl.when(has_right)
        def _():
            x_own(r, 0).wait_send()
            for dist in range(1, NT - 1):
                @pl.when(t >= dist)
                def _():
                    x_forward(r, 0, dist).wait_send()

        @pl.when(has_left)
        def _():
            x_own(r, 1).wait_send()
            for dist in range(1, NT - 1):
                @pl.when(t <= NT - 1 - dist)
                def _():
                    x_forward(r, 1, dist).wait_send()

        return z

    lax.fori_loop(0, NR, drain_x, 0)
    if qkv:
        pass_kv(6)
        pass_kv(7)

        @pl.when(is_end)
        def _():
            for p in range(NP):
                z_out(p).wait_send()

        @pl.when(is_mid)
        def _():
            for p in range(NP):
                zx(p, True).wait_send()
                zx(p, False).wait_recv()

        own_seg.wait()
        for i in range(3):
            seg_out(i).wait_send()
            seg_in(i).wait_recv()
        pltpu.make_async_copy(kv, kv_all.at[s], loc.at[2]).wait()

        @pl.when(yc == 0)
        def _():
            at = pl.ds(0, early)
            remote(kv.at[:, at], kv_all.at[s, :, at], kv_send.at[0], kv_yr.at[0], to_y).wait_send()

        @pl.when(c == 0)
        def _():
            remote(kv, kv_all.at[s], kv_send.at[1], kv_cr.at[0], to_sib).wait_send()

        def drain_kv(r, z):
            @pl.when(c == 1)
            def _():
                kv_row(r, sib, None, kv_fs.at[r], kv_cr.at[r]).wait_recv()

            @pl.when(yc == 1)
            def _():
                kv_row(r, ynb, to_sib, kv_fs.at[r], kv_fr.at[r]).wait_send()
                kv_row(r, diag, to_sib, kv_fs.at[r], kv_fr.at[r]).wait_recv()

            return z

        lax.fori_loop(0, NR, drain_kv, 0)


def _gather_call(qkv, x, w, seg, wo):
    R, C = x.shape
    N = w.shape[1]
    dma = pltpu.SemaphoreType.DMA
    hbm = pl.BlockSpec(memory_space=pltpu.HBM)
    vmem = pl.BlockSpec(memory_space=pltpu.VMEM)
    bf16 = jnp.bfloat16
    scratch = [pltpu.VMEM((NT, R, C), bf16), pltpu.VMEM((NT, C, N), bf16)]
    if qkv:
        heads = N // (3 * HEAD_DIM)
        out_shape = (
            jax.ShapeDtypeStruct((R, heads * HEAD_DIM), bf16),
            jax.ShapeDtypeStruct((NT, R, 2 * heads * HEAD_DIM), bf16),
            jax.ShapeDtypeStruct((NT,) + seg.shape, jnp.int32),
            jax.ShapeDtypeStruct(wo.shape, bf16),
        )
        out_specs = (vmem, hbm, hbm, hbm)
        scratch.append(pltpu.VMEM((R, 2 * heads * HEAD_DIM), bf16))
    else:
        out_shape = jax.ShapeDtypeStruct((R, N), bf16)
        out_specs = vmem
    scratch += [dma((4,)), dma((2, 3, NR)), dma((3, NR)), dma((3, NR)), dma((NP,)), dma((NP,)), dma((NP,)), dma((2, NP)),
                dma((NP,)), dma((NP,)), dma((NP,)), dma((2, NP))]
    if qkv:
        scratch += [dma((2,)), dma((NR,)), dma((NR,)), dma((NR,)), dma((NR,)), dma((3,)), dma((3,)), dma((NP,)), dma((NP,)), dma((NP,)), dma((NP,))]
    return pl.pallas_call(
        functools.partial(_gather_dot, qkv),
        out_shape=out_shape,
        in_specs=[hbm] * 4,
        out_specs=out_specs,
        scratch_shapes=scratch,
        compiler_params=pltpu.CompilerParams(collective_id=0 if qkv else 1, has_side_effects=True, vmem_limit_bytes=60 * MIB),
        cost_estimate=pl.CostEstimate(flops=2 * R * NT * C * N, bytes_accessed=2 * NT * (R * C + C * N), transcendentals=0),
        name="qkv_dot" if qkv else "out_dot",
    )(x, w, seg, wo)


def _attend_out(q_hbm, kv_hbm, seg_hbm, w_hbm, w2_hbm, y_hbm, q_ref, kv_ref, seg_ref, first_ref, sc0, sc1, m0, m1, l0, l1, acc_ref, xg, wg, wg2,
                y1, y2, loc, kv_sem, late_sem, w_send, w_recv, o_send, o_recv, e_send, e_recv, y_send, y_recv):
    R, C = q_hbm.shape
    N = w_hbm.shape[1]
    BQ = R // NB
    NH = N // (2 * NP)
    BK = 2 * BQ
    H = C // HEAD_DIM
    CP = 2 * HEAD_DIM
    per = C // CP
    NU = NB * per
    d, t, s = lax.axis_index("dp"), lax.axis_index("tp"), lax.axis_index("sp")
    yc, c = s // 2, s % 2
    sib, ynb, diag = s + 1 - 2 * c, s + 2 - 4 * yc, (2 - 2 * yc) + (1 - c)
    mesh_id = pl.DeviceIdType.MESH
    to_sib, to_y, to_x = (d, t, sib), (d, t, ynb), (1 - d, t, s)
    is_end = (t == 0) | (t == NT - 1)
    is_mid = jnp.logical_not(is_end)
    e, o = 3 * t - 3, 3 - t
    oe = 3 - e
    to_m, to_e, to_o = (d, (t + 3) // 3, s), (d, e, s), (d, o, s)
    bar = pltpu.get_barrier_semaphore()

    def greet(who):
        pl.semaphore_signal(bar, inc=1, device_id=who, device_id_type=mesh_id)

    def remote(src, dst, send, recv, who):
        return pltpu.make_async_remote_copy(src, dst, send, recv, device_id=who, device_id_type=mesh_id)

    def rows(b):
        return pl.ds(_mo(b, BQ), BQ)

    def mine(p):
        return pl.ds(_mo(2 * p + d, NH), NH)

    def other(p):
        return pl.ds(_mo(2 * p + 1 - d, NH), NH)

    def piece(k, u):
        return xg.at[k, pl.ds(_mo(u // per, BQ), BQ), pl.ds(_mo(u % per, CP), CP)]

    kinds = {
        "y": (s, mine, to_y, ynb, mine),
        "x": (ynb, mine, to_x, ynb, other),
        "sy": (ynb, mine, to_sib, diag, mine),
        "sx": (ynb, other, to_sib, diag, other),
    }
    number = {kind: i for i, kind in enumerate(kinds)}
    panels = ((w_hbm, wg), (w2_hbm, wg2))

    def w_out(i, kind, p):
        hbm, panel = panels[i]
        owner, cols, who, _, _ = kinds[kind]
        n = number[kind]
        src = hbm.at[:, cols(p)] if kind == "y" else panel.at[owner, :, cols(p)]
        return remote(src, panel.at[owner, :, cols(p)], w_send.at[i, n, p], w_recv.at[i, n, p], who)

    def w_in(i, kind, p):
        _, _, who, owner, cols = kinds[kind]
        n = number[kind]
        at = panels[i][1].at[owner, :, cols(p)]
        return remote(at, at, w_send.at[i, n, p], w_recv.at[i, n, p], who)

    def w_sib(i, owner):
        return remote(panels[i][0], panels[i][1].at[owner], loc.at[4 + i], loc.at[6 + i], to_sib)

    def w_own(i):
        return pltpu.make_async_copy(panels[i][0], panels[i][1].at[s], loc.at[2 + i])

    def end_piece(u, who):
        k = t if who is to_m else e
        return remote(piece(k, u), piece(k, u), e_send.at[u], e_recv.at[u], who)

    def own_piece(u):
        return remote(piece(t, u), piece(t, u), o_send.at[0, u], o_recv.at[0, u], to_o)

    def passed_piece(u):
        return remote(piece(e, u), piece(e, u), o_send.at[1, u], o_recv.at[1, u], to_o)

    def piece_in(i, u):
        k = o if i == 0 else oe
        return remote(piece(k, u), piece(k, u), o_send.at[i, u], o_recv.at[i, u], to_o)

    def y_out(r, who):
        return remote(y2.at[rows(r)], y_hbm.at[rows(r)], y_send.at[r], y_recv.at[r], who)

    q_copy = pltpu.make_async_copy(q_hbm, q_ref, loc.at[0])
    seg_copy = pltpu.make_async_copy(seg_hbm, seg_ref, loc.at[1])

    def kv_copy(h, k):
        return pltpu.make_async_copy(kv_hbm.at[k, :, pl.ds(_mo(h, CP), CP)], kv_ref.at[h, pl.ds(_mo(k, R), R)], kv_sem.at[h, k])

    seg_copy.start()
    q_copy.start()
    for h in range(H):
        for k in range(NT):
            @pl.when((k <= s) & (yc == 0) if h >= H - LATE and k < NT // 2 else k <= s)
            def _():
                kv_copy(h, k).start()

    greet(to_y)
    greet(to_sib)

    @pl.when(is_end)
    def _():
        greet(to_m)
        pl.semaphore_wait(bar, 3)

    @pl.when(is_mid)
    def _():
        for who in (to_e, to_o, to_x):
            greet(who)
        pl.semaphore_wait(bar, 5)

    def late_y(i):
        h = H - LATE + i
        return remote(kv_hbm.at[s, :, pl.ds(h * CP, CP)], kv_ref.at[h, pl.ds(_mo(s, R), R)], late_sem.at[0, i], late_sem.at[1, i], to_y)

    def late_kv(i, owner):
        at = kv_ref.at[H - LATE + i, pl.ds(_mo(owner, R), R)]
        return remote(at, at, late_sem.at[2, i], late_sem.at[3, i], to_sib)

    def late_y_in(i):
        at = kv_ref.at[H - LATE + i, pl.ds(_mo(ynb, R), R)]
        return remote(at, at, late_sem.at[0, i], late_sem.at[1, i], to_y)

    @pl.when(yc == 0)
    def _():
        for i in range(LATE):
            late_y(i).start()

    @pl.when(is_mid)
    def _():
        for i in (1, 0):
            for p in range(NP):
                w_out(i, "y", p).start()
        for i in (1, 0):
            w_sib(i, s).start()
            w_own(i).start()

    seg_copy.wait()
    seg = seg_ref[...]
    starts = [jnp.sum(jnp.where(seg < doc, 1.0, 0.0), axis=(0, 1), keepdims=True) for doc in range(1, 4)]

    def first_rows(b, z):
        row = (s * R + b * BQ + lax.broadcasted_iota(jnp.int32, (BQ, HEAD_DIM), 0)).astype(jnp.float32)
        out = jnp.zeros((BQ, HEAD_DIM), jnp.float32)
        for start in starts:
            out = jnp.where(start <= row, jnp.maximum(out, start), out)
        first_ref[pl.ds(_mo(b, BQ), BQ), :] = out.astype(jnp.int32)
        return z

    lax.fori_loop(0, NB, first_rows, 0)
    q_copy.wait()

    scale = LOG2E / HEAD_DIM ** 0.5
    sc, m_refs, l_refs = (sc0, sc1), (m0, m1), (l0, l1)

    def lane_groups(a, op):
        out = a[:, :HEAD_DIM]
        for g in range(1, a.shape[1] // HEAD_DIM):
            out = op(out, a[:, HEAD_DIM * g : HEAD_DIM * (g + 1)])
        return out

    def wide(a):
        return jnp.concatenate([a] * (BK // HEAD_DIM), axis=1)

    def attend(half, k, par, stages):
        full = 2 * s + half
        b, h = 2 * half + k // H, k % H
        q_at = pl.ds(_mo(b, BQ), BQ)
        b3, h3 = 2 * half + (k - 2) // H, (k - 2) % H
        if 1 in stages:
            m_refs[par][...] = jnp.full((BQ, HEAD_DIM), -3e38, jnp.float32)
        if 2 in stages:
            l_refs[1 - par][...] = jnp.zeros((BQ, HEAD_DIM), jnp.float32)
        if 3 in stages:
            acc_ref[...] = jnp.zeros((BQ, HEAD_DIM), jnp.float32)

        def tile(j, z, width, diagonal):
            if 3 in stages:
                acc = acc_ref[...]
                scale_l = wide(l_refs[par][...])
                for i in range(width):
                    p = (sc[par][j + i] * scale_l).astype(jnp.bfloat16)
                    acc += jnp.dot(p, kv_ref[h3, pl.ds(_mo(j + i, BK), BK), HEAD_DIM:], preferred_element_type=jnp.float32)
                acc_ref[...] = acc
            if 1 in stages:
                q = q_ref[q_at, pl.ds(_mo(h, HEAD_DIM), HEAD_DIM)]
                first = wide(first_ref[q_at, :])
                m = m_refs[par][...]
                for i in range(width):
                    a = lax.dot_general(q, kv_ref[h, pl.ds(_mo(j + i, BK), BK), :HEAD_DIM], (((1,), (1,)), ((), ())), preferred_element_type=jnp.float32)
                    key_id = (j + i) * BK + lax.broadcasted_iota(jnp.int32, (BQ, BK), 1)
                    seen = key_id >= first
                    if diagonal:
                        seen = seen & (key_id <= s * R + b * BQ + lax.broadcasted_iota(jnp.int32, (BQ, BK), 0))
                    a = jnp.where(seen, a, -jnp.inf)
                    sc[par][j + i] = a
                    m = jnp.maximum(m, lane_groups(a, jnp.maximum))
                m_refs[par][...] = m
            if 2 in stages:
                top = wide(m_refs[1 - par][...])
                l = l_refs[1 - par][...]
                for i in range(width):
                    w = jnp.exp2((sc[1 - par][j + i] - top) * scale)
                    sc[1 - par][j + i] = w
                    l += lane_groups(w, jnp.add)
                l_refs[1 - par][...] = l
            return z

        lax.fori_loop(0, s, lambda i, z: tile(2 * i, z, 2, False), 0)
        lax.fori_loop(0, half, lambda i, z: tile(2 * s, z, 1, False), 0)
        tile(full, 0, 1, True)
        if 1 in stages:
            m_refs[par][...] = jnp.broadcast_to(jnp.max(m_refs[par][...], axis=1, keepdims=True), (BQ, HEAD_DIM))
        if 2 in stages:
            l_refs[1 - par][...] = jnp.broadcast_to(1.0 / jnp.sum(l_refs[1 - par][...], axis=1, keepdims=True), (BQ, HEAD_DIM))
        if 3 in stages:
            xg[t, pl.ds(_mo(b3, BQ), BQ), pl.ds(_mo(h3, HEAD_DIM), HEAD_DIM)] = acc_ref[...].astype(jnp.bfloat16)

    def dot_rows(panel, out, r):
        acc = jnp.dot(xg[0, rows(r), :], panel[0], preferred_element_type=jnp.float32)
        for k in range(1, NT):
            acc += jnp.dot(xg[k, rows(r), :], panel[k], preferred_element_type=jnp.float32)
        out[rows(r), :] = acc.astype(jnp.bfloat16)

    def relay_piece(u):
        end_piece(u, to_e).wait_recv()
        passed_piece(u).start()

    def relay_w(i, kind, p):
        w_in(i, kind, p).wait_recv()
        if kind == "y":
            w_out(i, "x", p).start()
            w_out(i, "sy", p).start()
        else:
            w_out(i, "sx", p).start()

    plan = ((1, "y", 6), (1, "x", 11), (0, "y", 21), (0, "x", 26))
    steps = H * 2 + 2

    def after(half, k):
        g = half * steps + k
        for i in range(LATE):
            @pl.when((yc == 1) & (g == H - 2 - LATE + i))
            def _():
                late_y_in(i).wait_recv()
                late_kv(i, ynb).start()

        for i, kind, base in plan:
            @pl.when(is_mid & (g >= base) & (g < base + 4 * NP) & ((g - base) % 4 == 0))
            def _():
                relay_w(i, kind, (g - base) // 4)

    def finished(u):
        @pl.when(is_end)
        def _():
            end_piece(u, to_m).start()

        @pl.when(is_mid)
        def _():
            @pl.when(u >= 1)
            def _():
                relay_piece(u - 1)

            own_piece(u).start()

    def kv_here(half, k):
        @pl.when((half == 0) & (k < H))
        def _():
            for owner in range(NT):
                @pl.when((owner <= s) & ((yc == 0) | (k < H - LATE)) if owner < NT // 2 else owner <= s)
                def _():
                    kv_copy(k, owner).wait()
            for i in range(LATE):
                @pl.when((yc == 1) & (k == H - LATE + i))
                def _():
                    late_kv(i, diag).wait_recv()

    def panel_here(i):
        w_own(i).wait()
        w_sib(i, sib).wait_recv()
        for kind in ("sy", "sx"):
            for p in range(NP):
                w_in(i, kind, p).wait_recv()

    def end_columns(b, n):
        for u in range(n * per):
            piece_in(0, b * per + u).wait_recv()
            piece_in(1, b * per + u).wait_recv()
        def chunk(r, z):
            dot_rows(wg2, y2, r)

            @pl.when(r > b)
            def _():
                y_out(r - 1, to_e).start()

            return z

        lax.fori_loop(b, b + n, chunk, 0)

    def half_rows(half, z):
        kv_here(half, 0)
        attend(half, 0, 0, (1,))
        after(half, 0)
        kv_here(half, 1)
        attend(half, 1, 1, (1, 2))
        after(half, 1)

        def pair(i, z):
            for par in range(2):
                k = 2 * i + par
                kv_here(half, k)
                attend(half, k, par, (1, 2, 3))
                after(half, k)
            finished(half * 2 * per + i - 1)

            @pl.when(is_mid & (half == 1) & (i == 4))
            def _():
                panel_here(1)
                end_columns(0, 2)

            @pl.when(is_mid & (half == 1) & (i == 5))
            def _():
                y_out(1, to_e).start()

            @pl.when(is_mid & (half == 1) & (i == H - 1))
            def _():
                end_columns(2, 1)

            return z

        lax.fori_loop(1, H, pair, 0)
        attend(half, 2 * H, 0, (2, 3))
        after(half, 2 * H)

        @pl.when(is_mid & (half == 1))
        def _():
            y_out(2, to_e).start()

        attend(half, 2 * H + 1, 1, (3,))
        after(half, 2 * H + 1)
        finished(half * 2 * per + 2 * per - 1)
        return z

    lax.fori_loop(0, NB // 2, half_rows, 0)
    for i in range(LATE):
        @pl.when(yc == 0)
        def _():
            late_y(i).wait_send()

        @pl.when(yc == 1)
        def _():
            late_kv(i, ynb).wait_send()

    @pl.when(is_end)
    def _():
        def drain(u, z):
            end_piece(u, to_m).wait_send()
            return z

        lax.fori_loop(0, NU, drain, 0)
        for r in range(NB):
            y_out(r, to_m).wait_recv()

    @pl.when(is_mid)
    def _():
        relay_piece(NU - 1)
        for i, kind, base in plan:
            for p in range(NP):
                if base + 4 * p >= 2 * steps:
                    relay_w(i, kind, p)

        end_columns(3, 1)
        panel_here(0)
        y_out(NB - 1, to_e).start()

        def own_columns(r, z):
            dot_rows(wg, y1, r)
            return z

        lax.fori_loop(0, NB, own_columns, 0)
        own_y = pltpu.make_async_copy(y1, y_hbm, loc.at[0])
        own_y.start()

        def drain(u, z):
            own_piece(u).wait_send()
            passed_piece(u).wait_send()
            return z

        lax.fori_loop(0, NU, drain, 0)
        for r in range(NB):
            y_out(r, to_e).wait_send()
        for i in range(2):
            w_sib(i, s).wait_send()
            for kind in kinds:
                for p in range(NP):
                    w_out(i, kind, p).wait_send()
        own_y.wait()


def _attend_call(q, kv_all, seg_all, w, w2):
    R, C = q.shape
    N = w.shape[1]
    BQ = R // NB
    NU = NB * (C // (2 * HEAD_DIM))
    dma = pltpu.SemaphoreType.DMA
    hbm = pl.BlockSpec(memory_space=pltpu.HBM)
    bf16, f32 = jnp.bfloat16, jnp.float32
    stat = pltpu.VMEM((BQ, HEAD_DIM), f32)
    scores = pltpu.VMEM((NT * NB // 2, BQ, 2 * BQ), f32)
    return pl.pallas_call(
        _attend_out,
        out_shape=jax.ShapeDtypeStruct((R, N), bf16),
        in_specs=[hbm] * 5,
        out_specs=hbm,
        scratch_shapes=[
            pltpu.VMEM((R, C), bf16),
            pltpu.VMEM((C // HEAD_DIM, NT * R, 2 * HEAD_DIM), bf16),
            pltpu.VMEM(seg_all.shape, jnp.int32),
            pltpu.VMEM((R, HEAD_DIM), jnp.int32),
            scores, scores, stat, stat, stat, stat, stat,
            pltpu.VMEM((NT, R, C), bf16),
            pltpu.VMEM((NT, C, N), bf16),
            pltpu.VMEM((NT, C, N), bf16),
            pltpu.VMEM((R, N), bf16),
            pltpu.VMEM((R, N), bf16),
            dma((8,)), dma((C // HEAD_DIM, NT)), dma((4, LATE)), dma((2, 4, NP)), dma((2, 4, NP)), dma((2, NU)), dma((2, NU)), dma((NU,)), dma((NU,)),
            dma((NB,)), dma((NB,)),
        ],
        compiler_params=pltpu.CompilerParams(collective_id=1, has_side_effects=True, vmem_limit_bytes=62 * MIB),
        cost_estimate=pl.CostEstimate(flops=4 * R * NT * C * N, bytes_accessed=2 * NT * (R * C + C * N), transcendentals=R * NT * R * 4),
        name="attend_out",
    )(q, kv_all, seg_all, w, w2)


def solution(mesh):
    def local_block(x_blk, wqkv_blk, wout_blk, seg_blk):
        q, kv_all, seg_all, w2 = _gather_call(True, x_blk, wqkv_blk, seg_blk.reshape(-1, 128), wout_blk)
        return _attend_call(q, kv_all, seg_all.reshape(-1, 128), wout_blk, w2)

    row_spec = P(("dp", "sp"), "tp")
    return jax.shard_map(local_block, mesh=mesh, in_specs=(row_spec, P("sp", "tp"), P("sp", "tp"), P(("dp", "sp"))), out_specs=row_spec, check_vma=False)
```

```python
import functools

import jax
import jax.numpy as jnp
from jax import lax
from jax.experimental import pallas as pl
from jax.experimental.pallas import tpu as pltpu
from jax.sharding import PartitionSpec as P

HEAD_DIM = 128
NT = 4
NR = 8
NB = 4
AHEAD = 1
LATE = 1
NP = 4
LOG2E = 1.4426950408889634
MIB = 1024 * 1024


def _mo(i, n):
    return pl.multiple_of(i * n, n)


def _gather_dot(qkv, x_hbm, w_hbm, seg_hbm, wo_hbm, *refs):
    if qkv:
        q_ref, kv_all, seg_all, w2_hbm = refs[:4]
        refs = refs[4:]
    else:
        (y_ref,) = refs[:1]
        refs = refs[1:]
    xg, wg = refs[:2]
    refs = refs[2:]
    if qkv:
        kv = refs[0]
        refs = refs[1:]
    loc, xs, xl, xr, ws_own, ws_y, ws_x, ws_f, wr_own, wr_y, wr_x, wr_f = refs[:12]
    if qkv:
        kv_send, kv_yr, kv_cr, kv_fs, kv_fr, seg_s, seg_r, z_s, z_r, zx_s, zx_r = refs[12:]

    R, C = x_hbm.shape
    N = w_hbm.shape[1]
    RC, NG, NH = R // NR, N // NP, N // (2 * NP)
    d, t, s = lax.axis_index("dp"), lax.axis_index("tp"), lax.axis_index("sp")
    yc, c = s // 2, s % 2
    sib, ynb, diag = s + 1 - 2 * c, s + 2 - 4 * yc, (2 - 2 * yc) + (1 - c)
    mesh_id = pl.DeviceIdType.MESH
    to_sib, to_y, to_diag = (d, t, sib), (d, t, ynb), (d, t, diag)
    to_x = (1 - d, t, s)
    to_right, to_left = (d, t + 1, s), (d, t - 1, s)
    has_right, has_left = t < NT - 1, t > 0

    bar = pltpu.get_barrier_semaphore()

    def greet(who):
        pl.semaphore_signal(bar, inc=1, device_id=who, device_id_type=mesh_id)

    greet(to_sib)
    greet(to_y)
    greet(to_x)
    if qkv:
        greet(to_diag)

    @pl.when(has_right)
    def _():
        greet(to_right)

    @pl.when(has_left)
    def _():
        greet(to_left)

    base = 4 if qkv else 3

    @pl.when(has_right & has_left)
    def _():
        pl.semaphore_wait(bar, base + 2)

    @pl.when(jnp.logical_not(has_right & has_left))
    def _():
        pl.semaphore_wait(bar, base + 1)

    def remote(src, dst, send, recv, who):
        return pltpu.make_async_remote_copy(src, dst, send, recv, device_id=who, device_id_type=mesh_id)

    def w_own(p):
        cols = pl.ds(p * NG, NG)
        return remote(w_hbm.at[:, cols], wg.at[s, :, cols], ws_own.at[p], wr_own.at[p], to_sib)

    def w_own_in(p):
        cols = pl.ds(p * NG, NG)
        return remote(w_hbm.at[:, cols], wg.at[sib, :, cols], ws_own.at[p], wr_own.at[p], to_sib)

    def mine(p):
        return pl.ds(_mo(2 * p + d, NH), NH)

    def other(p):
        return pl.ds(_mo(2 * p + 1 - d, NH), NH)

    def w_y(p):
        return remote(w_hbm.at[:, mine(p)], wg.at[s, :, mine(p)], ws_y.at[p], wr_y.at[p], to_y)

    def w_y_in(p):
        return remote(w_hbm.at[:, mine(p)], wg.at[ynb, :, mine(p)], ws_y.at[p], wr_y.at[p], to_y)

    def w_x(p):
        return remote(wg.at[ynb, :, mine(p)], wg.at[ynb, :, mine(p)], ws_x.at[p], wr_x.at[p], to_x)

    def w_x_in(p):
        return remote(wg.at[ynb, :, other(p)], wg.at[ynb, :, other(p)], ws_x.at[p], wr_x.at[p], to_x)

    def w_f(p, which):
        cols = mine(p) if which == 0 else other(p)
        return remote(wg.at[ynb, :, cols], wg.at[ynb, :, cols], ws_f.at[which, p], wr_f.at[which, p], to_sib)

    def w_f_in(p, which):
        cols = mine(p) if which == 0 else other(p)
        return remote(wg.at[diag, :, cols], wg.at[diag, :, cols], ws_f.at[which, p], wr_f.at[which, p], to_sib)

    def rows(r):
        return pl.ds(_mo(r, RC), RC)

    def x_own(r, way):
        recv = xl if way == 0 else xr
        return remote(x_hbm.at[rows(r)], xg.at[t, rows(r)], xs.at[way, 0, r], recv.at[0, r], to_right if way == 0 else to_left)

    def x_arrive(r, way, dist):
        k = t - dist if way == 0 else t + dist
        recv = xl if way == 0 else xr
        return remote(xg.at[k, rows(r)], xg.at[k, rows(r)], xs.at[way, 0, r], recv.at[dist - 1, r], to_right if way == 0 else to_left)

    def x_forward(r, way, dist):
        k = t - dist if way == 0 else t + dist
        recv = xl if way == 0 else xr
        return remote(xg.at[k, rows(r)], xg.at[k, rows(r)], xs.at[way, dist, r], recv.at[dist, r], to_right if way == 0 else to_left)

    def send_own_x(r):
        @pl.when(has_right)
        def _():
            x_own(r, 0).start()

        @pl.when(has_left)
        def _():
            x_own(r, 1).start()

    def relay_x(i):
        for dist in range(1, NT):
            r = i - (dist - 1)
            for way in range(2):
                here = (t >= dist) if way == 0 else (t <= NT - 1 - dist)

                @pl.when(here & (r >= 0) & (r < NR))
                def _():
                    x_arrive(r, way, dist).wait_recv()
                    if dist < NT - 1:
                        @pl.when(has_right if way == 0 else has_left)
                        def _():
                            x_forward(r, way, dist).start()

            if dist == 1:
                @pl.when(jnp.int32(i + AHEAD) < NR)
                def _():
                    send_own_x(i + AHEAD)

    own_x = pltpu.make_async_copy(x_hbm, xg.at[t], loc.at[0])
    own_w = pltpu.make_async_copy(w_hbm, wg.at[s], loc.at[1])
    for r in range(AHEAD):
        send_own_x(r)
    for p in range(NP):
        w_y(p).start()
    for p in range(NP):
        w_own(p).start()
    own_x.start()
    own_w.start()
    if qkv:
        own_seg = pltpu.make_async_copy(seg_hbm, seg_all.at[s], loc.at[3])
        own_seg.start()
        peers = ((to_sib, sib), (to_y, ynb), (to_diag, diag))

        def seg_out(i):
            return remote(seg_hbm, seg_all.at[s], seg_s.at[i], seg_r.at[i], peers[i][0])

        def seg_in(i):
            return remote(seg_hbm, seg_all.at[peers[i][1]], seg_s.at[i], seg_r.at[i], peers[i][0])

        for i in range(3):
            seg_out(i).start()

    def unit(r, p):
        cols = pl.ds(_mo(p, NG), NG)
        acc = jnp.dot(xg[0, rows(r), :], wg[0, :, cols], preferred_element_type=jnp.float32)
        for k in range(1, NT):
            acc += jnp.dot(xg[k, rows(r), :], wg[k, :, cols], preferred_element_type=jnp.float32)
        out = acc.astype(jnp.bfloat16)
        if qkv:
            for h in range(2):
                at = 3 * HEAD_DIM * h
                q_ref[rows(r), pl.ds(pl.multiple_of(p * (2 * HEAD_DIM) + h * HEAD_DIM, HEAD_DIM), HEAD_DIM)] = out[:, at : at + HEAD_DIM]
                kv[rows(r), pl.ds(_mo(2 * p + h, 2 * HEAD_DIM), 2 * HEAD_DIM)] = out[:, at + HEAD_DIM : at + 3 * HEAD_DIM]
        else:
            y_ref[rows(r), cols] = out

    if qkv:
        early = kv.shape[1] - LATE * 2 * HEAD_DIM

    def kv_cols(p):
        return pl.ds(_mo(p, 4 * HEAD_DIM), 4 * HEAD_DIM)

    def kv_unit(r, p, who, send, recv):
        return remote(kv.at[rows(r), kv_cols(p)], kv_all.at[s, rows(r), kv_cols(p)], send, recv, who)

    def send_unit(r, p):
        pltpu.make_async_copy(kv.at[rows(r), kv_cols(p)], kv_all.at[s, rows(r), kv_cols(p)], loc.at[2]).start()

        @pl.when((yc == 0) & (p < NP - 1))
        def _():
            kv_unit(r, p, to_y, kv_send.at[0], kv_yr.at[r]).start()

        if LATE == 1:
            @pl.when((yc == 0) & (p == NP - 1))
            def _():
                at = pl.ds((NP - 1) * 4 * HEAD_DIM, 2 * HEAD_DIM)
                remote(kv.at[rows(r), at], kv_all.at[s, rows(r), at], kv_send.at[0], kv_yr.at[r], to_y).start()

        @pl.when(c == 0)
        def _():
            kv_unit(r, p, to_sib, kv_send.at[1], kv_cr.at[r]).start()

    def do_units(work):
        for n, f in work:
            def body(u, z, f=f):
                unit(*f(u))
                if qkv:
                    @pl.when(u > 0)
                    def _():
                        send_unit(*f(u - 1))
                return z
            lax.fori_loop(0, n, body, 0)
            if qkv:
                send_unit(*f(jnp.int32(n - 1)))

    def kv_row(r, owner, who, send, recv):
        at = pl.ds(0, early if who is not None else kv.shape[1])
        who = to_sib if who is None else who
        return remote(kv_all.at[owner, rows(r), at], kv_all.at[owner, rows(r), at], send, recv, who)

    def pass_kv(r):
        if qkv:
            @pl.when(yc == 1)
            def _():
                kv_row(r, ynb, to_y, kv_fs.at[r], kv_yr.at[r]).wait_recv()
                kv_row(r, ynb, to_sib, kv_fs.at[r], kv_fr.at[r]).start()

    is_end = (t == 0) | (t == NT - 1)
    is_mid = jnp.logical_not(is_end)
    N2 = wo_hbm.shape[1] // (2 * NP)

    def half_cols(p, mine_cols):
        return pl.ds(_mo(2 * p + d, N2) if mine_cols else _mo(2 * p + 1 - d, N2), N2)

    def z_out(p):
        at = half_cols(p, True)
        return remote(wo_hbm.at[:, at], w2_hbm.at[:, at], z_s.at[p], z_r.at[p], (d, (t + 3) // 3, s))

    def z_in(p):
        at = half_cols(p, True)
        return remote(w2_hbm.at[:, at], w2_hbm.at[:, at], z_s.at[p], z_r.at[p], to_x)

    def zx(p, mine_cols):
        at = half_cols(p, mine_cols)
        return remote(w2_hbm.at[:, at], w2_hbm.at[:, at], zx_s.at[p], zx_r.at[p], to_x)

    def relay_w(i):
        if qkv and i < NP:
            @pl.when(is_end)
            def _():
                z_out(i).start()
        if i < NP:
            w_y_in(i).wait_recv()
            w_x(i).start()
            w_f(i, 0).start()
        if 1 <= i <= NP:
            w_x_in(i - 1).wait_recv()
            w_f(i - 1, 1).start()
            p = i - 1
            if p == 0:
                own_x.wait()
                own_w.wait()
            w_own_in(p).wait_recv()
            w_f_in(p, 0).wait_recv()
            w_f_in(p, 1).wait_recv()

    LAG = NT - 2
    relay_x(jnp.int32(0))
    for i in range(NP + 1):
        relay_x(jnp.int32(i + 1))
        relay_w(i)
        if i == 2:
            do_units([(4, lambda u: (u // 2, u % 2))])
        if i == 3:
            do_units([(2, lambda u: (u, 2)), (3, lambda u: (2, u))])
        if i == 4:
            do_units([(3, lambda u: (u, 3)), (4, lambda u: (3, u))])

    def late(i, z):
        relay_x(i)
        @pl.when(i >= NP + 3)
        def _():
            pass_kv(2 * (i - NP - 3))
            pass_kv(2 * (i - NP - 3) + 1)

        @pl.when(is_mid & (i < NP + 4))
        def _():
            for p in range(2):
                z_in(2 * (i - NP - 2) + p).wait_recv()
                zx(2 * (i - NP - 2) + p, True).start()

        do_units([(NP, lambda u: (i - LAG, u))])
        return z

    lax.fori_loop(NP + 2, NR + LAG, late, 0)

    for p in range(NP):
        w_own(p).wait_send()
        w_y(p).wait_send()
        w_x(p).wait_send()
        w_f(p, 0).wait_send()
        w_f(p, 1).wait_send()

    def drain_x(r, z):
        @pl.when(has_right)
        def _():
            x_own(r, 0).wait_send()
            for dist in range(1, NT - 1):
                @pl.when(t >= dist)
                def _():
                    x_forward(r, 0, dist).wait_send()

        @pl.when(has_left)
        def _():
            x_own(r, 1).wait_send()
            for dist in range(1, NT - 1):
                @pl.when(t <= NT - 1 - dist)
                def _():
                    x_forward(r, 1, dist).wait_send()

        return z

    lax.fori_loop(0, NR, drain_x, 0)
    if qkv:
        pass_kv(6)
        pass_kv(7)

        @pl.when(is_end)
        def _():
            for p in range(NP):
                z_out(p).wait_send()

        @pl.when(is_mid)
        def _():
            for p in range(NP):
                zx(p, True).wait_send()
                zx(p, False).wait_recv()

        own_seg.wait()
        for i in range(3):
            seg_out(i).wait_send()
            seg_in(i).wait_recv()
        pltpu.make_async_copy(kv, kv_all.at[s], loc.at[2]).wait()

        @pl.when(yc == 0)
        def _():
            at = pl.ds(0, early)
            remote(kv.at[:, at], kv_all.at[s, :, at], kv_send.at[0], kv_yr.at[0], to_y).wait_send()

        @pl.when(c == 0)
        def _():
            remote(kv, kv_all.at[s], kv_send.at[1], kv_cr.at[0], to_sib).wait_send()

        def drain_kv(r, z):
            @pl.when(c == 1)
            def _():
                kv_row(r, sib, None, kv_fs.at[r], kv_cr.at[r]).wait_recv()

            @pl.when(yc == 1)
            def _():
                kv_row(r, ynb, to_sib, kv_fs.at[r], kv_fr.at[r]).wait_send()
                kv_row(r, diag, to_sib, kv_fs.at[r], kv_fr.at[r]).wait_recv()

            return z

        lax.fori_loop(0, NR, drain_kv, 0)


def _gather_call(qkv, x, w, seg, wo):
    R, C = x.shape
    N = w.shape[1]
    dma = pltpu.SemaphoreType.DMA
    hbm = pl.BlockSpec(memory_space=pltpu.HBM)
    vmem = pl.BlockSpec(memory_space=pltpu.VMEM)
    bf16 = jnp.bfloat16
    scratch = [pltpu.VMEM((NT, R, C), bf16), pltpu.VMEM((NT, C, N), bf16)]
    if qkv:
        heads = N // (3 * HEAD_DIM)
        out_shape = (
            jax.ShapeDtypeStruct((R, heads * HEAD_DIM), bf16),
            jax.ShapeDtypeStruct((NT, R, 2 * heads * HEAD_DIM), bf16),
            jax.ShapeDtypeStruct((NT,) + seg.shape, jnp.int32),
            jax.ShapeDtypeStruct(wo.shape, bf16),
        )
        out_specs = (vmem, hbm, hbm, hbm)
        scratch.append(pltpu.VMEM((R, 2 * heads * HEAD_DIM), bf16))
    else:
        out_shape = jax.ShapeDtypeStruct((R, N), bf16)
        out_specs = vmem
    scratch += [dma((4,)), dma((2, 3, NR)), dma((3, NR)), dma((3, NR)), dma((NP,)), dma((NP,)), dma((NP,)), dma((2, NP)),
                dma((NP,)), dma((NP,)), dma((NP,)), dma((2, NP))]
    if qkv:
        scratch += [dma((2,)), dma((NR,)), dma((NR,)), dma((NR,)), dma((NR,)), dma((3,)), dma((3,)), dma((NP,)), dma((NP,)), dma((NP,)), dma((NP,))]
    return pl.pallas_call(
        functools.partial(_gather_dot, qkv),
        out_shape=out_shape,
        in_specs=[hbm] * 4,
        out_specs=out_specs,
        scratch_shapes=scratch,
        compiler_params=pltpu.CompilerParams(collective_id=0 if qkv else 1, has_side_effects=True, vmem_limit_bytes=60 * MIB),
        cost_estimate=pl.CostEstimate(flops=2 * R * NT * C * N, bytes_accessed=2 * NT * (R * C + C * N), transcendentals=0),
        name="qkv_dot" if qkv else "out_dot",
    )(x, w, seg, wo)


def _attend_out(q_hbm, kv_hbm, seg_hbm, w_hbm, w2_hbm, y_hbm, q_ref, kv_ref, seg_ref, first_ref, sc0, sc1, m0, m1, l0, l1, acc_ref, xg, wg, wg2,
                y1, y2, loc, kv_sem, late_sem, w_send, w_recv, o_send, o_recv, e_send, e_recv, y_send, y_recv):
    R, C = q_hbm.shape
    N = w_hbm.shape[1]
    BQ = R // NB
    NH = N // (2 * NP)
    BK = 2 * BQ
    H = C // HEAD_DIM
    CP = 2 * HEAD_DIM
    per = C // CP
    NU = NB * per
    d, t, s = lax.axis_index("dp"), lax.axis_index("tp"), lax.axis_index("sp")
    yc, c = s // 2, s % 2
    sib, ynb, diag = s + 1 - 2 * c, s + 2 - 4 * yc, (2 - 2 * yc) + (1 - c)
    mesh_id = pl.DeviceIdType.MESH
    to_sib, to_y, to_x = (d, t, sib), (d, t, ynb), (1 - d, t, s)
    is_end = (t == 0) | (t == NT - 1)
    is_mid = jnp.logical_not(is_end)
    e, o = 3 * t - 3, 3 - t
    oe = 3 - e
    to_m, to_e, to_o = (d, (t + 3) // 3, s), (d, e, s), (d, o, s)
    bar = pltpu.get_barrier_semaphore()

    def greet(who):
        pl.semaphore_signal(bar, inc=1, device_id=who, device_id_type=mesh_id)

    def remote(src, dst, send, recv, who):
        return pltpu.make_async_remote_copy(src, dst, send, recv, device_id=who, device_id_type=mesh_id)

    def rows(b):
        return pl.ds(_mo(b, BQ), BQ)

    def mine(p):
        return pl.ds(_mo(2 * p + d, NH), NH)

    def other(p):
        return pl.ds(_mo(2 * p + 1 - d, NH), NH)

    def piece(k, u):
        return xg.at[k, pl.ds(_mo(u // per, BQ), BQ), pl.ds(_mo(u % per, CP), CP)]

    kinds = {
        "y": (s, mine, to_y, ynb, mine),
        "x": (ynb, mine, to_x, ynb, other),
        "sy": (ynb, mine, to_sib, diag, mine),
        "sx": (ynb, other, to_sib, diag, other),
    }
    number = {kind: i for i, kind in enumerate(kinds)}
    panels = ((w_hbm, wg), (w2_hbm, wg2))

    def w_out(i, kind, p):
        hbm, panel = panels[i]
        owner, cols, who, _, _ = kinds[kind]
        n = number[kind]
        src = hbm.at[:, cols(p)] if kind == "y" else panel.at[owner, :, cols(p)]
        return remote(src, panel.at[owner, :, cols(p)], w_send.at[i, n, p], w_recv.at[i, n, p], who)

    def w_in(i, kind, p):
        _, _, who, owner, cols = kinds[kind]
        n = number[kind]
        at = panels[i][1].at[owner, :, cols(p)]
        return remote(at, at, w_send.at[i, n, p], w_recv.at[i, n, p], who)

    def w_sib(i, owner):
        return remote(panels[i][0], panels[i][1].at[owner], loc.at[4 + i], loc.at[6 + i], to_sib)

    def w_own(i):
        return pltpu.make_async_copy(panels[i][0], panels[i][1].at[s], loc.at[2 + i])

    def end_piece(u, who):
        k = t if who is to_m else e
        return remote(piece(k, u), piece(k, u), e_send.at[u], e_recv.at[u], who)

    def own_piece(u):
        return remote(piece(t, u), piece(t, u), o_send.at[0, u], o_recv.at[0, u], to_o)

    def passed_piece(u):
        return remote(piece(e, u), piece(e, u), o_send.at[1, u], o_recv.at[1, u], to_o)

    def piece_in(i, u):
        k = o if i == 0 else oe
        return remote(piece(k, u), piece(k, u), o_send.at[i, u], o_recv.at[i, u], to_o)

    def y_out(r, who):
        return remote(y2.at[rows(r)], y_hbm.at[rows(r)], y_send.at[r], y_recv.at[r], who)

    q_copy = pltpu.make_async_copy(q_hbm, q_ref, loc.at[0])
    seg_copy = pltpu.make_async_copy(seg_hbm, seg_ref, loc.at[1])

    def kv_copy(h, k):
        return pltpu.make_async_copy(kv_hbm.at[k, :, pl.ds(_mo(h, CP), CP)], kv_ref.at[h, pl.ds(_mo(k, R), R)], kv_sem.at[h, k])

    seg_copy.start()
    q_copy.start()
    for h in range(H):
        for k in range(NT):
            @pl.when((k <= s) & (yc == 0) if h >= H - LATE and k < NT // 2 else k <= s)
            def _():
                kv_copy(h, k).start()

    greet(to_y)
    greet(to_sib)

    @pl.when(is_end)
    def _():
        greet(to_m)
        pl.semaphore_wait(bar, 3)

    @pl.when(is_mid)
    def _():
        for who in (to_e, to_o, to_x):
            greet(who)
        pl.semaphore_wait(bar, 5)

    def late_y(i):
        h = H - LATE + i
        return remote(kv_hbm.at[s, :, pl.ds(h * CP, CP)], kv_ref.at[h, pl.ds(_mo(s, R), R)], late_sem.at[0, i], late_sem.at[1, i], to_y)

    def late_kv(i, owner):
        at = kv_ref.at[H - LATE + i, pl.ds(_mo(owner, R), R)]
        return remote(at, at, late_sem.at[2, i], late_sem.at[3, i], to_sib)

    def late_y_in(i):
        at = kv_ref.at[H - LATE + i, pl.ds(_mo(ynb, R), R)]
        return remote(at, at, late_sem.at[0, i], late_sem.at[1, i], to_y)

    @pl.when(yc == 0)
    def _():
        for i in range(LATE):
            late_y(i).start()

    @pl.when(is_mid)
    def _():
        for i in (1, 0):
            for p in range(NP):
                w_out(i, "y", p).start()
        for i in (1, 0):
            w_sib(i, s).start()
            w_own(i).start()

    seg_copy.wait()
    seg = seg_ref[...]
    starts = [jnp.sum(jnp.where(seg < doc, 1.0, 0.0), axis=(0, 1), keepdims=True) for doc in range(1, 4)]

    def first_rows(b, z):
        row = (s * R + b * BQ + lax.broadcasted_iota(jnp.int32, (BQ, HEAD_DIM), 0)).astype(jnp.float32)
        out = jnp.zeros((BQ, HEAD_DIM), jnp.float32)
        for start in starts:
            out = jnp.where(start <= row, jnp.maximum(out, start), out)
        first_ref[pl.ds(_mo(b, BQ), BQ), :] = out.astype(jnp.int32)
        return z

    lax.fori_loop(0, NB, first_rows, 0)
    q_copy.wait()

    scale = LOG2E / HEAD_DIM ** 0.5
    sc, m_refs, l_refs = (sc0, sc1), (m0, m1), (l0, l1)

    def lane_groups(a, op):
        out = a[:, :HEAD_DIM]
        for g in range(1, a.shape[1] // HEAD_DIM):
            out = op(out, a[:, HEAD_DIM * g : HEAD_DIM * (g + 1)])
        return out

    def wide(a):
        return jnp.concatenate([a] * (BK // HEAD_DIM), axis=1)

    def attend(half, k, par, stages):
        full = 2 * s + half
        b, h = 2 * half + k // H, k % H
        q_at = pl.ds(_mo(b, BQ), BQ)
        b3, h3 = 2 * half + (k - 2) // H, (k - 2) % H
        if 1 in stages:
            m_refs[par][...] = jnp.full((BQ, HEAD_DIM), -3e38, jnp.float32)
        if 2 in stages:
            l_refs[1 - par][...] = jnp.zeros((BQ, HEAD_DIM), jnp.float32)
        if 3 in stages:
            acc_ref[...] = jnp.zeros((BQ, HEAD_DIM), jnp.float32)

        def tile(j, z, width, diagonal):
            if 3 in stages:
                acc = acc_ref[...]
                scale_l = wide(l_refs[par][...])
                for i in range(width):
                    p = (sc[par][j + i] * scale_l).astype(jnp.bfloat16)
                    acc += jnp.dot(p, kv_ref[h3, pl.ds(_mo(j + i, BK), BK), HEAD_DIM:], preferred_element_type=jnp.float32)
                acc_ref[...] = acc
            if 1 in stages:
                q = q_ref[q_at, pl.ds(_mo(h, HEAD_DIM), HEAD_DIM)]
                first = wide(first_ref[q_at, :])
                m = m_refs[par][...]
                for i in range(width):
                    a = lax.dot_general(q, kv_ref[h, pl.ds(_mo(j + i, BK), BK), :HEAD_DIM], (((1,), (1,)), ((), ())), preferred_element_type=jnp.float32)
                    key_id = (j + i) * BK + lax.broadcasted_iota(jnp.int32, (BQ, BK), 1)
                    seen = key_id >= first
                    if diagonal:
                        seen = seen & (key_id <= s * R + b * BQ + lax.broadcasted_iota(jnp.int32, (BQ, BK), 0))
                    a = jnp.where(seen, a, -jnp.inf)
                    sc[par][j + i] = a
                    m = jnp.maximum(m, lane_groups(a, jnp.maximum))
                m_refs[par][...] = m
            if 2 in stages:
                top = wide(m_refs[1 - par][...])
                l = l_refs[1 - par][...]
                for i in range(width):
                    w = jnp.exp2((sc[1 - par][j + i] - top) * scale)
                    sc[1 - par][j + i] = w
                    l += lane_groups(w, jnp.add)
                l_refs[1 - par][...] = l
            return z

        lax.fori_loop(0, s, lambda i, z: tile(2 * i, z, 2, False), 0)
        lax.fori_loop(0, half, lambda i, z: tile(2 * s, z, 1, False), 0)
        tile(full, 0, 1, True)
        if 1 in stages:
            m_refs[par][...] = jnp.broadcast_to(jnp.max(m_refs[par][...], axis=1, keepdims=True), (BQ, HEAD_DIM))
        if 2 in stages:
            l_refs[1 - par][...] = jnp.broadcast_to(1.0 / jnp.sum(l_refs[1 - par][...], axis=1, keepdims=True), (BQ, HEAD_DIM))
        if 3 in stages:
            xg[t, pl.ds(_mo(b3, BQ), BQ), pl.ds(_mo(h3, HEAD_DIM), HEAD_DIM)] = acc_ref[...].astype(jnp.bfloat16)

    def dot_rows(panel, out, r):
        acc = jnp.dot(xg[0, rows(r), :], panel[0], preferred_element_type=jnp.float32)
        for k in range(1, NT):
            acc += jnp.dot(xg[k, rows(r), :], panel[k], preferred_element_type=jnp.float32)
        out[rows(r), :] = acc.astype(jnp.bfloat16)

    def relay_piece(u):
        end_piece(u, to_e).wait_recv()
        passed_piece(u).start()

    def relay_w(i, kind, p):
        w_in(i, kind, p).wait_recv()
        if kind == "y":
            w_out(i, "x", p).start()
            w_out(i, "sy", p).start()
        else:
            w_out(i, "sx", p).start()

    plan = ((1, "y", 6), (1, "x", 11), (0, "y", 21), (0, "x", 26))
    steps = H * 2 + 2

    def after(half, k):
        g = half * steps + k
        for i in range(LATE):
            @pl.when((yc == 1) & (g == H - 2 - LATE + i))
            def _():
                late_y_in(i).wait_recv()
                late_kv(i, ynb).start()

        for i, kind, base in plan:
            @pl.when(is_mid & (g >= base) & (g < base + 4 * NP) & ((g - base) % 4 == 0))
            def _():
                relay_w(i, kind, (g - base) // 4)

    def finished(u):
        @pl.when(is_end)
        def _():
            end_piece(u, to_m).start()

        @pl.when(is_mid)
        def _():
            @pl.when(u >= 1)
            def _():
                relay_piece(u - 1)

            own_piece(u).start()

    def kv_here(half, k):
        @pl.when((half == 0) & (k < H))
        def _():
            for owner in range(NT):
                @pl.when((owner <= s) & ((yc == 0) | (k < H - LATE)) if owner < NT // 2 else owner <= s)
                def _():
                    kv_copy(k, owner).wait()
            for i in range(LATE):
                @pl.when((yc == 1) & (k == H - LATE + i))
                def _():
                    late_kv(i, diag).wait_recv()

    def panel_here(i):
        w_own(i).wait()
        w_sib(i, sib).wait_recv()
        for kind in ("sy", "sx"):
            for p in range(NP):
                w_in(i, kind, p).wait_recv()

    def end_columns(b, n):
        for u in range(n * per):
            piece_in(0, b * per + u).wait_recv()
            piece_in(1, b * per + u).wait_recv()
        def chunk(r, z):
            dot_rows(wg2, y2, r)

            @pl.when(r > b)
            def _():
                y_out(r - 1, to_e).start()

            return z

        lax.fori_loop(b, b + n, chunk, 0)

    def half_rows(half, z):
        kv_here(half, 0)
        attend(half, 0, 0, (1,))
        after(half, 0)
        kv_here(half, 1)
        attend(half, 1, 1, (1, 2))
        after(half, 1)

        def pair(i, z):
            for par in range(2):
                k = 2 * i + par
                kv_here(half, k)
                attend(half, k, par, (1, 2, 3))
                after(half, k)
            finished(half * 2 * per + i - 1)

            @pl.when(is_mid & (half == 1) & (i == 4))
            def _():
                panel_here(1)
                end_columns(0, 2)

            @pl.when(is_mid & (half == 1) & (i == 5))
            def _():
                y_out(1, to_e).start()

            @pl.when(is_mid & (half == 1) & (i == H - 1))
            def _():
                end_columns(2, 1)

            return z

        lax.fori_loop(1, H, pair, 0)
        attend(half, 2 * H, 0, (2, 3))
        after(half, 2 * H)

        @pl.when(is_mid & (half == 1))
        def _():
            y_out(2, to_e).start()

        attend(half, 2 * H + 1, 1, (3,))
        after(half, 2 * H + 1)
        finished(half * 2 * per + 2 * per - 1)
        return z

    lax.fori_loop(0, NB // 2, half_rows, 0)
    for i in range(LATE):
        @pl.when(yc == 0)
        def _():
            late_y(i).wait_send()

        @pl.when(yc == 1)
        def _():
            late_kv(i, ynb).wait_send()

    @pl.when(is_end)
    def _():
        def drain(u, z):
            end_piece(u, to_m).wait_send()
            return z

        lax.fori_loop(0, NU, drain, 0)
        for r in range(NB):
            y_out(r, to_m).wait_recv()

    @pl.when(is_mid)
    def _():
        relay_piece(NU - 1)
        for i, kind, base in plan:
            for p in range(NP):
                if base + 4 * p >= 2 * steps:
                    relay_w(i, kind, p)

        end_columns(3, 1)
        panel_here(0)
        y_out(NB - 1, to_e).start()

        def own_columns(r, z):
            dot_rows(wg, y1, r)
            return z

        lax.fori_loop(0, NB, own_columns, 0)
        own_y = pltpu.make_async_copy(y1, y_hbm, loc.at[0])
        own_y.start()

        def drain(u, z):
            own_piece(u).wait_send()
            passed_piece(u).wait_send()
            return z

        lax.fori_loop(0, NU, drain, 0)
        for r in range(NB):
            y_out(r, to_e).wait_send()
        for i in range(2):
            w_sib(i, s).wait_send()
            for kind in kinds:
                for p in range(NP):
                    w_out(i, kind, p).wait_send()
        own_y.wait()


def _attend_call(q, kv_all, seg_all, w, w2):
    R, C = q.shape
    N = w.shape[1]
    BQ = R // NB
    NU = NB * (C // (2 * HEAD_DIM))
    dma = pltpu.SemaphoreType.DMA
    hbm = pl.BlockSpec(memory_space=pltpu.HBM)
    bf16, f32 = jnp.bfloat16, jnp.float32
    stat = pltpu.VMEM((BQ, HEAD_DIM), f32)
    scores = pltpu.VMEM((NT * NB // 2, BQ, 2 * BQ), f32)
    return pl.pallas_call(
        _attend_out,
        out_shape=jax.ShapeDtypeStruct((R, N), bf16),
        in_specs=[hbm] * 5,
        out_specs=hbm,
        scratch_shapes=[
            pltpu.VMEM((R, C), bf16),
            pltpu.VMEM((C // HEAD_DIM, NT * R, 2 * HEAD_DIM), bf16),
            pltpu.VMEM(seg_all.shape, jnp.int32),
            pltpu.VMEM((R, HEAD_DIM), jnp.int32),
            scores, scores, stat, stat, stat, stat, stat,
            pltpu.VMEM((NT, R, C), bf16),
            pltpu.VMEM((NT, C, N), bf16),
            pltpu.VMEM((NT, C, N), bf16),
            pltpu.VMEM((R, N), bf16),
            pltpu.VMEM((R, N), bf16),
            dma((8,)), dma((C // HEAD_DIM, NT)), dma((4, LATE)), dma((2, 4, NP)), dma((2, 4, NP)), dma((2, NU)), dma((2, NU)), dma((NU,)), dma((NU,)),
            dma((NB,)), dma((NB,)),
        ],
        compiler_params=pltpu.CompilerParams(collective_id=1, has_side_effects=True, vmem_limit_bytes=62 * MIB),
        cost_estimate=pl.CostEstimate(flops=4 * R * NT * C * N, bytes_accessed=2 * NT * (R * C + C * N), transcendentals=R * NT * R * 4),
        name="attend_out",
    )(q, kv_all, seg_all, w, w2)


def solution(mesh):
    def local_block(x_blk, wqkv_blk, wout_blk, seg_blk):
        q, kv_all, seg_all, w2 = _gather_call(True, x_blk, wqkv_blk, seg_blk.reshape(-1, 128), wout_blk)
        return _attend_call(q, kv_all, seg_all.reshape(-1, 128), wout_blk, w2)

    row_spec = P(("dp", "sp"), "tp")
    return jax.shard_map(local_block, mesh=mesh, in_specs=(row_spec, P("sp", "tp"), P("sp", "tp"), P(("dp", "sp"))), out_specs=row_spec, check_vma=False)
```
